128 devices in a mesh: seq: 16 (over y, x), head: 8 (over z, core).
Axes of the slice: x: 4, y: 4, z: 4, core: 2. Of those that a mesh axis runs over, the one named last changes fastest.
Arguments:
- segment_input: bfloat16 [2, 4096, 3584], P(None, 'seq'), may hold values from -16 to 16
- doc_ids: int32 [2, 4096], replicated, may hold values from 0 to 3, never falling along the last dimension, each value on 1 to 2048 neighbouring positions
- memory: bfloat16 [32, 3584], replicated, may hold values from -16 to 16
- gain: bfloat16 [3584], replicated, may hold values from 0.099609375 to 1.8984375
- w_query: bfloat16 [3584, 4096], P(None, 'head'), may hold values from -4 to 4
- w_key: bfloat16 [3584, 2048], P(None, 'head'), may hold values from -4 to 4
- w_value: bfloat16 [3584, 2048], P(None, 'head'), may hold values from -0.09375 to 0.09375
- w_out: bfloat16 [4096, 3584], P(None, 'head'), may hold values from -0.09375 to 0.09375
- mem_proj: bfloat16 [3584, 3584], P('head'), may hold values from -4 to 4
Outputs:
- hidden: bfloat16 [2, 4096, 3584], P(None, 'seq', 'head')
- new_memory: bfloat16 [32, 3584], replicated
The draws below stay inside these ranges and needn't reach their ends.
Inputs may be any that keep to these rules, and one draw needn't show every extreme that they name: `doc_ids`: ids never fall along a segment; each document has 1 to 2048 tokens.
All inputs are finite; a program needn't handle non-finite values.
Results may differ from the reference program's by a relative error of at most 0.02.
Values may be sent and summed in bfloat16 or wider, within the bound.
No kernel may reach another device: no remote copies, remote signals or barrier semaphores. Data moves between devices by JAX's collectives and lax.ppermute only.
A program may use at most 128 MiB of HBM per device.

```python
import math
import jax
import jax.numpy as jnp
import numpy as np
from jax import lax

D = 3584
HEADS = 16
KV_HEADS = 8
HD = 256
M = 32
SEGS = 2
TOKENS = 4096


def drawn_rows(row_key, row_count):
    return jnp.clip(jax.random.normal(jax.random.fold_in(row_key, 1), (row_count, D), jnp.float32), -6.0, 6.0)


def draw_segment_input(key, part):
    pieces = []
    for segment in range(SEGS):
        row_key = jax.random.fold_in(key, 500 + segment)
        pieces.append(drawn_rows(row_key, TOKENS))
    return jnp.stack(pieces, axis=0).astype(jnp.bfloat16)


def draw_memory(key, part):
    row_key = jax.random.fold_in(key, 700)
    result = drawn_rows(row_key, M)
    return result.astype(jnp.bfloat16)


def draw_w_query(key, part):
    weights = jnp.clip(jax.random.normal(jax.random.fold_in(key, 9201), (D, HEADS, HD), jnp.float32), -4.0, 4.0) * D ** (-0.5)
    return weights.reshape(D, HEADS * HD).astype(jnp.bfloat16)


def draw_w_key(key, part):
    weights = jnp.clip(jax.random.normal(jax.random.fold_in(key, 9202), (D, KV_HEADS, HD), jnp.float32), -4.0, 4.0) * D ** (-0.5)
    return weights.reshape(D, KV_HEADS * HD).astype(jnp.bfloat16)


def draw_mem_proj(key, part):
    weights = jnp.clip(jax.random.normal(jax.random.fold_in(key, 9203), (D, D), jnp.float32), -4.0, 4.0) * D ** (-0.5)
    return weights.astype(jnp.bfloat16)


def steps_of(own_key, dims, split, smallest, high):
    def one(dim, parts):
        steps = jax.random.uniform(jax.random.fold_in(jax.random.fold_in(own_key, 6), dim), (parts,), jnp.float32, smallest / len(split), high / len(split))
        return jnp.repeat(jnp.exp(steps), dims[dim] // parts).reshape((-1,) + (1,) * (len(dims) - dim - 1))

    loudness = one(*split[0])
    for cut in split[1:]:
        loudness = loudness * one(*cut)
    return loudness


def split_up(number_of, total, bound, lean):
    weights = [(1 << 20) // math.isqrt(rank ** lean) + 1 for rank in range(2, number_of + 1)]
    rest, counts = total - bound - (number_of - 1), [1] * (number_of - 1)
    while rest > 0:
        candidates = [i for i in range(number_of - 1) if counts[i] < bound]
        pool, budget = sum([weights[i] for i in candidates]), rest
        for i in candidates:
            extra = min(bound - counts[i], max(1, budget * weights[i] // pool), rest)
            counts[i] = counts[i] + extra
            rest = rest - extra
    return np.array([bound] + counts)


def ragged_sizes(rng, amount, total, most, slope):
    if amount == 2:
        one = jax.random.randint(rng, (), max(1, total - most), min(most, total - 1) + 1)
        return jnp.stack([one, total - one])
    sizes = jnp.asarray(split_up(amount, total, most, slope), jnp.int32)
    twos = (amount - 1) // 2
    source_of, taker = sizes[1:1 + 2 * twos:2], sizes[2:2 + 2 * twos:2]
    room = jnp.minimum(source_of - 1, most - taker)
    moved = jax.random.randint(jax.random.fold_in(rng, 1), (twos,), 0, 1 << 20) % (room + 1)
    sizes = sizes.at[1:1 + 2 * twos:2].set(source_of - moved).at[2:2 + 2 * twos:2].set(taker + moved)
    return sizes[jax.random.permutation(jax.random.fold_in(rng, 2), amount)]


def normal_values(own_key, extent, spread, limit, cuts=(), held_as=jnp.bfloat16):
    values = jax.random.normal(own_key, extent, jnp.float32) * spread
    if len(cuts) > 0:
        values = steps_of(own_key, extent, cuts, -0.22, 0.18) * values
    return jnp.clip(values, min=-limit, max=limit).astype(held_as)


def setup_inputs(seed: int = 0) -> dict:
    splits = jax.random.split(jax.random.key(seed), 10)
    return {
        "segment_input": draw_segment_input(jax.random.fold_in(splits[9], 71), 0),
        "doc_ids": jax.vmap(lambda own: jnp.searchsorted(jnp.cumsum(ragged_sizes(own, 4, TOKENS, TOKENS // 2, 0)), jnp.arange(TOKENS), side="right"))(jax.random.split(splits[1], SEGS)).reshape((SEGS, TOKENS)).astype(jnp.int32),
        "memory": draw_memory(jax.random.fold_in(splits[9], 71), 0),
        "gain": jnp.clip(1.0 + 0.18 * jax.random.normal(splits[3], (D,), jnp.float32), 0.099609375, 1.8984375).astype(jnp.bfloat16),
        "w_query": draw_w_query(jax.random.fold_in(splits[9], 71), 0),
        "w_key": draw_w_key(jax.random.fold_in(splits[9], 71), 0),
        "w_value": normal_values(splits[6], (D, KV_HEADS * HD), D ** -0.5, 0.09375, ((1, 8),)),
        "w_out": normal_values(splits[7], (HEADS * HD, D), (HEADS * HD) ** -0.5, 0.09375, ((1, 8),)),
        "mem_proj": draw_mem_proj(jax.random.fold_in(splits[9], 71), 0),
    }


def rms_norm(rows, gain):
    values = rows.astype(jnp.float32)
    scaled = values * lax.rsqrt(lax.optimization_barrier(jnp.mean(values * values, axis=-1, keepdims=True)) + 1e-06)
    return (scaled * gain.astype(jnp.float32)).astype(jnp.bfloat16)

def reference(segment_input, doc_ids, memory, gain, w_query, w_key, w_value, w_out, mem_proj):
    mem = memory
    outputs = []
    scale = jnp.float32(HD ** (-0.5))
    for seg in range(SEGS):
        tokens = segment_input[seg]
        docs = doc_ids[seg]
        normed_x = rms_norm(tokens, gain)
        normed_m = rms_norm(mem, gain)
        rows_all = jnp.concatenate([normed_x, normed_m], axis=0)
        query = jnp.dot(rows_all, w_query, preferred_element_type=jnp.float32).astype(jnp.bfloat16)
        keys = jnp.dot(rows_all, w_key, preferred_element_type=jnp.float32).astype(jnp.bfloat16)
        values = jnp.dot(rows_all, w_value, preferred_element_type=jnp.float32).astype(jnp.bfloat16)
        rows = TOKENS + M
        query = query.reshape(rows, KV_HEADS, 2, HD).transpose(1, 0, 2, 3)
        keys = jnp.concatenate([keys[TOKENS:], keys[:TOKENS]], axis=0).reshape(rows, KV_HEADS, HD).transpose(1, 0, 2)
        values = jnp.concatenate([values[TOKENS:], values[:TOKENS]], axis=0).reshape(rows, KV_HEADS, HD).transpose(1, 0, 2)
        position = jnp.arange(TOKENS, dtype=jnp.int32)
        allowed = (position[None, :] <= position[:, None]) & (docs[None, :] == docs[:, None])
        token_mask = jnp.concatenate([jnp.ones((TOKENS, M), dtype=bool), allowed], axis=1)
        mask = jnp.concatenate([token_mask, jnp.ones((M, rows), dtype=bool)], axis=0)

        def one_group(operands):
            group_query, group_keys, group_values = operands
            scores = jnp.einsum('rgd,kd->grk', group_query.astype(jnp.float32), group_keys.astype(jnp.float32)) * scale
            scores = jnp.where(mask[None], scores, -1e+30)
            peak = lax.optimization_barrier(jnp.max(scores, axis=-1, keepdims=True))
            weights = jnp.where(mask[None], jnp.exp(scores - peak), 0.0)
            total = lax.optimization_barrier(jnp.sum(weights, axis=-1))
            mixed = jnp.einsum('grk,kd->grd', weights.astype(jnp.bfloat16).astype(jnp.float32), group_values.astype(jnp.float32))
            return mixed / total[..., None]
        attended = lax.map(one_group, (query, keys, values))
        attended = attended.transpose(2, 0, 1, 3).reshape(rows, HEADS * HD).astype(jnp.bfloat16)
        attn_tok = attended[:TOKENS]
        attn_mem = attended[TOKENS:]
        outputs.append((tokens.astype(jnp.float32) + jnp.dot(attn_tok, w_out, preferred_element_type=jnp.float32)).astype(jnp.bfloat16))
        mem_out = (mem.astype(jnp.float32) + jnp.dot(attn_mem, w_out, preferred_element_type=jnp.float32)).astype(jnp.bfloat16)
        mem = jnp.dot(mem_out, mem_proj, preferred_element_type=jnp.float32).astype(jnp.bfloat16)
    return (jnp.stack(outputs, axis=0), mem)
```

```python
import functools
import math

import jax
import jax.numpy as jnp
from jax import lax
from jax.experimental import pallas as pl
from jax.experimental.pallas import tpu as pltpu
from jax.sharding import PartitionSpec as P

D = 3584
HD = 256
M = 32
ROWS = 256
COLS = 448
HALF = D // 2
KC = 512
SHAPE = 4
LOG2E_SCALE = math.log2(math.e) / 16.0
LOW = -1e30
BF = jnp.bfloat16
F32 = jnp.float32


WHOLE = pl.BlockSpec(memory_space=pltpu.VMEM)
SCALARS = pl.BlockSpec(memory_space=pltpu.SMEM)


def params(mib, **kw):
    return pltpu.CompilerParams(vmem_limit_bytes=mib * 1024 * 1024, **kw)


def dot(a, b):
    return jnp.dot(a, b, preferred_element_type=F32)


def dot_t(a, b):
    return lax.dot_general(a, b, (((1,), (1,)), ((), ())), preferred_element_type=F32)


def normed(rows, gain):
    v = rows.astype(F32)
    r = lax.rsqrt(jnp.mean(v * v, axis=-1, keepdims=True) + 1e-6)
    return (v * r * gain.astype(F32)).astype(BF)


def column(row):
    return jnp.broadcast_to(row, (128, row.shape[1])).T[:, :1]


def as_row(col):
    return jnp.broadcast_to(col, (col.shape[0], 128)).T[:1, :]


def attend(score_list, value_list):
    peak = functools.reduce(jnp.maximum, [jnp.max(s, axis=1, keepdims=True) for s in score_list])
    peak = jnp.maximum(peak, -1e29)
    total = 0.0
    mixed = 0.0
    for s, v in zip(score_list, value_list):
        p = jnp.exp2(s - peak)
        total = total + jnp.sum(p, axis=1, keepdims=True)
        mixed = mixed + dot(p.astype(BF), v)
    some = total > 0.0
    out = mixed / jnp.where(some, total, 1.0)
    return out, jnp.where(some, peak + jnp.log2(jnp.where(some, total, 1.0)), LOW)


def memory_part(qkvm, keys, values, first, out_ref):
    for g in range(2):
        q = qkvm[:, g * HD : (g + 1) * HD]
        s = dot_t(q, keys) * LOG2E_SCALE
        sm = dot_t(q, qkvm[:, 2 * HD : 3 * HD]) * LOG2E_SCALE
        sm = jnp.where(first, sm, LOW)
        out, lse = attend([s, sm], [values, qkvm[:, 3 * HD :]])
        hi = lse.astype(BF)
        lo = (lse - hi.astype(F32)).astype(BF)
        lane = lax.broadcasted_iota(jnp.int32, (M, 128), 1)
        stats = jnp.where(lane == 0, hi.astype(F32), jnp.where(lane == 1, lo.astype(F32), 0.0))
        out_ref[g * M : (g + 1) * M, :HD] = out.astype(BF)
        out_ref[g * M : (g + 1) * M, HD:] = stats.astype(BF)


def project_kernel(with_mem, ids, x_ref, *refs):
    if with_mem:
        mem_ref, gain_ref, wq, wk, wv, q_ref, kv_ref, qkvm_ref, part_ref, xn, acc = refs
    else:
        gain_ref, wq, wk, wv, q_ref, kv_ref, xn, acc = refs
    k = pl.program_id(0)

    @pl.when(k == 0)
    def _():
        def chunk(r, carry):
            rows = pl.ds(r * 32, 32)
            xn[rows, :] = normed(x_ref[0, rows, :], gain_ref[...])
            return carry

        lax.fori_loop(0, ROWS // 32, chunk, 0)
        if with_mem:
            xn[ROWS:, :] = normed(mem_ref[...], gain_ref[...])
        acc[...] = jnp.zeros_like(acc)

    a = xn[:, pl.ds(pl.multiple_of(k * KC, KC), KC)]
    acc[:, : 2 * HD] += dot(a, wq[...])
    acc[:, 2 * HD : 3 * HD] += dot(a, wk[...])
    acc[:, 3 * HD :] += dot(a, wv[...])

    @pl.when(k == D // KC - 1)
    def _():
        q_ref[...] = acc[:ROWS, : 2 * HD].astype(BF)
        kv_ref[...] = acc[:ROWS, 2 * HD :].astype(BF)
        if with_mem:
            qkvm_ref[...] = acc[ROWS:, :].astype(BF)
            memory_part(
                qkvm_ref[...], kv_ref[:, :HD], kv_ref[:, HD:], ids[0] + ids[1] == 0, part_ref
            )


def project(ids, x, seg, mem, gain, wq, wk, wv):
    with_mem = mem is not None
    rows = ROWS + (M if with_mem else 0)
    full = lambda k: (0, 0)
    in_specs = [SCALARS, pl.BlockSpec((1, ROWS, D), lambda k: (seg, 0, 0))]
    args = [ids, x]
    if with_mem:
        in_specs.append(pl.BlockSpec((M, D), full))
        args.append(mem)
    in_specs += [
        pl.BlockSpec((1, D), full),
        pl.BlockSpec((KC, 2 * HD), lambda k: (k, 0)),
        pl.BlockSpec((KC, HD), lambda k: (k, 0)),
        pl.BlockSpec((KC, HD), lambda k: (k, 0)),
    ]
    args += [gain, wq, wk, wv]
    shapes = [(ROWS, 2 * HD), (ROWS, 2 * HD)]
    if with_mem:
        shapes += [(M, 4 * HD), (2 * M, HD + 128)]
    return pl.pallas_call(
        functools.partial(project_kernel, with_mem),
        grid=(D // KC,),
        in_specs=in_specs,
        out_specs=[pl.BlockSpec(s, full) for s in shapes],
        out_shape=[jax.ShapeDtypeStruct(s, BF) for s in shapes],
        scratch_shapes=[pltpu.VMEM((rows, D), BF), pltpu.VMEM((rows, 4 * HD), F32)],
        compiler_params=params(24),
        cost_estimate=pl.CostEstimate(
            flops=2 * rows * D * 4 * HD, bytes_accessed=10 * 1024 * 1024, transcendentals=rows
        ),
        name="project",
    )(*args)


def memory_project_kernel(ids, own, other, gain, wq, wk, wv, kv, qkvm_ref, part_ref, whole_ref):
    c = ids[3]
    whole_ref[:, pl.ds(pl.multiple_of(c * HALF, 128), HALF)] = own[...]
    whole_ref[:, pl.ds(pl.multiple_of((1 - c) * HALF, 128), HALF)] = other[...]
    a = normed(whole_ref[...], gain[...])
    qkvm_ref[:, : 2 * HD] = dot(a, wq[...]).astype(BF)
    qkvm_ref[:, 2 * HD : 3 * HD] = dot(a, wk[...]).astype(BF)
    qkvm_ref[:, 3 * HD :] = dot(a, wv[...]).astype(BF)
    memory_part(qkvm_ref[...], kv[:, :HD], kv[:, HD:], ids[0] + ids[1] == 0, part_ref)


def memory_project(ids, own, other, gain, wq, wk, wv, kv):
    return pl.pallas_call(
        memory_project_kernel,
        in_specs=[SCALARS] + [WHOLE] * 7,
        out_specs=[WHOLE] * 3,
        out_shape=[
            jax.ShapeDtypeStruct((M, 4 * HD), BF),
            jax.ShapeDtypeStruct((2 * M, HD + 128), BF),
            jax.ShapeDtypeStruct((M, D), BF),
        ],
        compiler_params=params(20),
        cost_estimate=pl.CostEstimate(
            flops=2 * 256 * D * 4 * HD, bytes_accessed=8 * 1024 * 1024, transcendentals=M
        ),
        name="memory_project",
    )(ids, own, other, gain, wq, wk, wv, kv)


def memory_combine_kernel(last, a, b, c, d, out_ref):
    parts = [r[...].astype(F32) for r in (a, b, c, d)]
    lses = [p[:, HD : HD + 1] + p[:, HD + 1 : HD + 2] for p in parts]
    peak = functools.reduce(jnp.maximum, lses)
    ws = [jnp.exp2(s - peak) for s in lses]
    total = ws[0] + ws[1] + ws[2] + ws[3]
    out = sum(w * p[:, :HD] for w, p in zip(ws, parts)) / total
    if last:
        out_ref[:, :HD] = out[:M].astype(BF)
        out_ref[:, HD:] = out[M:].astype(BF)
    else:
        lse = peak + jnp.log2(total)
        hi = lse.astype(BF).astype(F32)
        lane = lax.broadcasted_iota(jnp.int32, (2 * M, 128), 1)
        stats = jnp.where(lane == 0, hi, jnp.where(lane == 1, lse - hi, 0.0))
        out_ref[:, :HD] = out.astype(BF)
        out_ref[:, HD:] = stats.astype(BF)


def memory_combine(parts, last):
    shape = (M, 2 * HD) if last else (2 * M, HD + 128)
    return pl.pallas_call(
        functools.partial(memory_combine_kernel, last),
        in_specs=[WHOLE] * 4,
        out_specs=WHOLE,
        out_shape=jax.ShapeDtypeStruct(shape, BF),
        compiler_params=params(4),
        cost_estimate=pl.CostEstimate(flops=10**8, bytes_accessed=10**5, transcendentals=256),
        name="memory_combine",
    )(*parts)


def memory_write_kernel(ids, p0, p1, p2, p3, cols, w_out, proj, keep_ref, send_ref):
    z, c = ids[2], ids[3]
    acc = cols[...].astype(F32)
    for k, p in enumerate((p0, p1, p2, p3)):
        for e in range(2):
            h = lax.rem(z - k + SHAPE, SHAPE) * 2 + (c if e == 0 else 1 - c)
            w = w_out[pl.ds(pl.multiple_of(h * 2 * HD, 2 * HD), 2 * HD), :]
            acc = acc + dot(p[e], w)
    a = acc.astype(BF)
    keep_ref[...] = dot(a, proj[:, pl.ds(pl.multiple_of(c * HALF, 128), HALF)]).astype(BF)
    send_ref[...] = dot(a, proj[:, pl.ds(pl.multiple_of((1 - c) * HALF, 128), HALF)]).astype(BF)


def memory_write(ids, pairs, cols, w_out, proj):
    return pl.pallas_call(
        memory_write_kernel,
        in_specs=[SCALARS] + [WHOLE] * 7,
        out_specs=[WHOLE] * 2,
        out_shape=[jax.ShapeDtypeStruct((M, HALF), BF)] * 2,
        compiler_params=params(20),
        cost_estimate=pl.CostEstimate(
            flops=2 * 256 * D * 8 * COLS, bytes_accessed=8 * 1024 * 1024, transcendentals=0
        ),
        name="memory_write",
    )(ids, *pairs, cols, w_out, proj)


def token_kernel(ids, docs, q0, q1, q2, q3, kva, kvb, kvc, qkvm, o0, o1, o2, o3, kvs, kcode):
    x, y = ids[0], ids[1]
    lane = lax.broadcasted_iota(jnp.int32, (1, ROWS), 1).astype(F32)
    for n, ref in enumerate((kva, kvb, kvc)):
        kvs[n * ROWS : (n + 1) * ROWS, :] = ref[...]
        block = (y - 2 + n) * SHAPE + x
        start = jnp.maximum(block, 0) * ROWS
        doc = docs[0, :, pl.ds(pl.multiple_of(start, ROWS), ROWS)].astype(F32)
        code = doc * 4096.0 + lane + start.astype(F32)
        kcode[:, n * ROWS : (n + 1) * ROWS] = jnp.where(block >= 0, code, -1.0)
    kv_m = qkvm[:, 2 * HD :]
    for d, (q_ref, o_ref) in enumerate(zip((q0, q1, q2, q3), (o0, o1, o2, o3))):
        start = (y * SHAPE + lax.rem(x - d + SHAPE, SHAPE)) * ROWS
        doc = docs[0, :, pl.ds(pl.multiple_of(start, ROWS), ROWS)].astype(F32)
        low = column(doc * 4096.0)
        high = column(doc * 4096.0 + lane + start.astype(F32))
        if d == 0:
            codes = kcode[...]
            keys = kvs[...]
        else:
            at = jnp.where(x >= d, 0, ROWS)
            at = pl.multiple_of(at, ROWS)
            codes = kcode[:, pl.ds(at, 2 * ROWS)]
            keys = kvs[pl.ds(at, 2 * ROWS), :]
        valid = (codes >= low) & (codes <= high)
        for g in range(2):
            q = q_ref[:, g * HD : (g + 1) * HD]
            scores = [jnp.where(valid, dot_t(q, keys[:, :HD]) * LOG2E_SCALE, LOW)]
            values = [keys[:, HD:]]
            if d == 0:
                scores.append(dot_t(q, kv_m[:, :HD]) * LOG2E_SCALE)
                values.append(kv_m[:, HD:])
            out, lse = attend(scores, values)
            row = as_row(lse)
            hi = row.astype(BF).astype(F32)
            sub = lax.broadcasted_iota(jnp.int32, (16, ROWS), 0)
            stats = jnp.where(sub == 0, hi, jnp.where(sub == 1, row - hi, 0.0))
            o_ref[:ROWS, g * HD : (g + 1) * HD] = out.astype(BF)
            o_ref[ROWS:, g * HD : (g + 1) * HD] = stats.astype(BF)


def token_attention(ids, docs, seg, qs, kva, kvb, kvc, qkvm):
    return pl.pallas_call(
        token_kernel,
        grid=(1,),
        in_specs=[SCALARS, pl.BlockSpec((1, 1, docs.shape[-1]), lambda k: (seg, 0, 0))]
        + [pl.BlockSpec((ROWS, 2 * HD), lambda k: (0, 0))] * 7
        + [pl.BlockSpec((M, 4 * HD), lambda k: (0, 0))],
        out_specs=[pl.BlockSpec((ROWS + 16, 2 * HD), lambda k: (0, 0))] * 4,
        out_shape=[jax.ShapeDtypeStruct((ROWS + 16, 2 * HD), BF)] * 4,
        scratch_shapes=[pltpu.VMEM((3 * ROWS, 2 * HD), BF), pltpu.VMEM((1, 3 * ROWS), F32)],
        compiler_params=params(24),
        cost_estimate=pl.CostEstimate(
            flops=3 * 10**9, bytes_accessed=4 * 10**6, transcendentals=10**6
        ),
        name="token_attention",
    )(ids, docs, *qs, kva, kvb, kvc, qkvm)


def token_combine_kernel(a, b, c, d, out_ref):
    refs = (a, b, c, d)
    for g in range(2):
        lanes = slice(g * HD, (g + 1) * HD)
        lses = []
        for r in refs:
            tail = r[ROWS:, lanes].astype(F32)
            lses.append(tail[0:1, :] + tail[1:2, :])
        peak = functools.reduce(jnp.maximum, lses)
        ws = [jnp.exp2(s - peak) for s in lses]
        total = ws[0] + ws[1] + ws[2] + ws[3]
        out = sum(column(w / total) * r[:ROWS, lanes].astype(F32) for w, r in zip(ws, refs))
        out_ref[:, lanes] = out.astype(BF)


def token_combine(parts):
    return pl.pallas_call(
        token_combine_kernel,
        in_specs=[WHOLE] * 4,
        out_specs=WHOLE,
        out_shape=jax.ShapeDtypeStruct((ROWS, 2 * HD), BF),
        compiler_params=params(12),
        cost_estimate=pl.CostEstimate(flops=5 * 10**8, bytes_accessed=10**6, transcendentals=4096),
        name="token_combine",
    )(*parts)


def token_out_kernel(ids, *refs):
    blocks, cols, w_out, out_ref = refs[:8], refs[8], refs[9], refs[-1]
    z, c = ids[2], ids[3]
    acc = cols[0].astype(F32)
    for n, ref in enumerate(blocks):
        k, e = n // 2, n % 2
        h = lax.rem(z - k + SHAPE, SHAPE) * 2 + (c if e == 0 else 1 - c)
        w = w_out[pl.ds(pl.multiple_of(h * 2 * HD, 2 * HD), 2 * HD), :]
        acc = acc + dot(ref[...], w)
    out_ref[0] = acc.astype(BF)


def token_out(ids, blocks, cols, seg, w_out, before):
    full = lambda k: (0, 0)
    in_specs = (
        [SCALARS]
        + [pl.BlockSpec((ROWS, 2 * HD), full)] * 8
        + [pl.BlockSpec((1, ROWS, COLS), lambda k: (seg, 0, 0)), WHOLE]
    )
    args = [ids, *blocks, cols, w_out]
    aliases = {}
    if before is not None:
        in_specs.append(pl.BlockSpec(memory_space=pl.ANY))
        args.append(before)
        aliases = {len(args) - 1: 0}
    return pl.pallas_call(
        token_out_kernel,
        grid=(1,),
        in_specs=in_specs,
        out_specs=pl.BlockSpec((1, ROWS, COLS), lambda k: (seg, 0, 0)),
        out_shape=jax.ShapeDtypeStruct((2, ROWS, COLS), BF),
        input_output_aliases=aliases,
        compiler_params=params(24),
        cost_estimate=pl.CostEstimate(
            flops=2 * ROWS * 4096 * COLS, bytes_accessed=6 * 10**6, transcendentals=0
        ),
        name="token_out",
    )(*args)


def x_shift(v, d):
    return lax.ppermute(
        v, "seq", [(i, i // SHAPE * SHAPE + (i + d) % SHAPE) for i in range(SHAPE * SHAPE)]
    )


def y_ring(v, d):
    n = SHAPE * SHAPE
    return lax.ppermute(v, "seq", [(i, (i + d * SHAPE) % n) for i in range(n)])


def y_later(v, d):
    n = SHAPE * SHAPE
    return lax.ppermute(v, "seq", [(i, i + d * SHAPE) for i in range(n - d * SHAPE)])


def z_shift(v, d):
    return lax.ppermute(v, "head", [(i, (i + 2 * d) % 8) for i in range(8)])


def other_core(v):
    return lax.ppermute(v, "head", [(i, i ^ 1) for i in range(8)])


def memory_tail(ids, part, cols, w_out, proj):
    part = memory_combine([part] + [x_shift(part, d) for d in (1, 3, 2)], False)
    attn = memory_combine([part] + [y_ring(part, d) for d in (1, 3, 2)], True)
    pair = jnp.stack([attn, other_core(attn)])
    pairs = [pair] + [z_shift(pair, d) for d in (1, 2, 3)]
    keep, send = memory_write(ids, pairs, cols, w_out, proj)
    both = (keep.astype(F32) + other_core(send).astype(F32)).astype(BF)
    terms = [both] + [z_shift(both, d) for d in (1, 2, 3)]
    own = sum(t.astype(F32) for t in terms).astype(BF)
    return own, other_core(own)


def per_device(segment_input, doc_ids, memory, gain, w_query, w_key, w_value, w_out, mem_proj):
    i = lax.axis_index("seq")
    h = lax.axis_index("head")
    ids = jnp.stack([i % SHAPE, i // SHAPE, h // 2, h % 2]).astype(jnp.int32)
    gain = gain.reshape(1, D)
    docs = doc_ids.reshape(2, 1, -1)

    q0, kv0, qkvm0, part0 = project(ids, segment_input, 0, memory, gain, w_query, w_key, w_value)
    mem_cols0 = lax.dynamic_slice_in_dim(memory, h * COLS, COLS, 1)
    q1, kv1 = project(ids, segment_input, 1, None, gain, w_query, w_key, w_value)
    cols = lax.dynamic_slice_in_dim(segment_input, h * COLS, COLS, 2)

    def attention(seg, q, kv, qkvm):
        kvb, kva = y_later(kv, 1), y_later(kv, 2)
        qs = [q] + [x_shift(q, d) for d in (1, 2, 3)]
        return token_attention(ids, docs, seg, qs, kva, kvb, kv, qkvm)

    def output(seg, parts, before):
        parts = [parts[0]] + [x_shift(parts[d], SHAPE - d) for d in (1, 2, 3)]
        attn = token_combine(parts)
        blocks = []
        for piece in [attn] + [z_shift(attn, d) for d in (1, 2, 3)]:
            blocks += [piece, other_core(piece)]
        return token_out(ids, blocks, cols, seg, w_out, before)

    own, other = memory_tail(ids, part0, mem_cols0, w_out, mem_proj)
    qkvm1, part1, mem1 = memory_project(ids, own, other, gain, w_query, w_key, w_value, kv1)
    mem_cols1 = lax.dynamic_slice_in_dim(mem1, h * COLS, COLS, 1)
    hidden = output(0, attention(0, q0, kv0, qkvm0), None)
    hidden = output(1, attention(1, q1, kv1, qkvm1), hidden)
    own, other = memory_tail(ids, part1, mem_cols1, w_out, mem_proj)
    swap = h % 2 == 1
    new_memory = jnp.concatenate(
        [jnp.where(swap, other, own), jnp.where(swap, own, other)], axis=1
    )
    return hidden, new_memory


def solution(mesh):
    return jax.shard_map(
        per_device,
        mesh=mesh,
        in_specs=(
            P(None, "seq", None),
            P(),
            P(),
            P(),
            P(None, "head"),
            P(None, "head"),
            P(None, "head"),
            P(None, "head"),
            P("head", None),
        ),
        out_specs=(P(None, "seq", "head"), P()),
        check_vma=False,
    )
```

```python
import functools
import math

import jax
import jax.numpy as jnp
from jax import lax
from jax.experimental import pallas as pl
from jax.experimental.pallas import tpu as pltpu
from jax.sharding import PartitionSpec as P


D = 3584
HD = 256
M = 32
ROWS = 256
COLS = 448
HALF = D // 2
KC = 512
SHAPE = 4
LOG2E_SCALE = math.log2(math.e) / 16.0
LOW = -1e30
BF = jnp.bfloat16
F32 = jnp.float32


WHOLE = pl.BlockSpec(memory_space=pltpu.VMEM)


def params(mib, **kw):
    return pltpu.CompilerParams(vmem_limit_bytes=mib * 1024 * 1024, **kw)


def dot(a, b):
    return jnp.dot(a, b, preferred_element_type=F32)


def dot_t(a, b):
    return lax.dot_general(a, b, (((1,), (1,)), ((), ())), preferred_element_type=F32)


def normed(rows, gain):
    v = rows.astype(F32)
    r = lax.rsqrt(jnp.mean(v * v, axis=-1, keepdims=True) + 1e-6)
    return (v * r * gain.astype(F32)).astype(BF)


def column(row):
    return jnp.broadcast_to(row, (128, row.shape[1])).T[:, :1]


def as_row(col):
    return jnp.broadcast_to(col, (col.shape[0], 128)).T[:1, :]


def attend(score_list, value_list):
    peak = functools.reduce(jnp.maximum, [jnp.max(s, axis=1, keepdims=True) for s in score_list])
    peak = jnp.maximum(peak, -1e29)
    total = 0.0
    mixed = 0.0
    for s, v in zip(score_list, value_list):
        p = jnp.exp2(s - peak)
        total = total + jnp.sum(p, axis=1, keepdims=True)
        mixed = mixed + dot(p.astype(BF), v)
    some = total > 0.0
    out = mixed / jnp.where(some, total, 1.0)
    return out, jnp.where(some, peak + jnp.log2(jnp.where(some, total, 1.0)), LOW)


def memory_part(qkvm, key_blocks, first, out_ref):
    for g in range(2):
        q = qkvm[:, g * HD : (g + 1) * HD]
        scores = [dot_t(q, kv[:, :HD]) * LOG2E_SCALE for kv in key_blocks]
        sm = dot_t(q, qkvm[:, 2 * HD : 3 * HD]) * LOG2E_SCALE
        scores.append(jnp.where(first, sm, LOW))
        out, lse = attend(scores, [kv[:, HD:] for kv in key_blocks] + [qkvm[:, 3 * HD :]])
        hi = lse.astype(BF)
        lo = (lse - hi.astype(F32)).astype(BF)
        lane = lax.broadcasted_iota(jnp.int32, (M, 128), 1)
        stats = jnp.where(lane == 0, hi.astype(F32), jnp.where(lane == 1, lo.astype(F32), 0.0))
        out_ref[g * M : (g + 1) * M, :HD] = out.astype(BF)
        out_ref[g * M : (g + 1) * M, HD:] = stats.astype(BF)


def place():
    i = lax.axis_index("seq")
    h = lax.axis_index("head")
    return i % SHAPE, i // SHAPE, h // 2, h % 2


def scaled_chunk(x, gain, squares, rows, first):
    v = x.astype(F32)
    sq = v * v
    part = sq[:, :128]
    for n in range(1, KC // 128):
        part = part + sq[:, n * 128 : (n + 1) * 128]
    squares[rows, :] = part if first else squares[rows, :] + part
    return (v * gain).astype(BF)


def norm_of(squares):
    return lax.rsqrt(jnp.sum(squares[...], axis=1, keepdims=True) / D + 1e-6)


def accumulate(acc, a, ws, first):
    at = 0
    for w in ws:
        span = slice(at, at + w.shape[1])
        part = dot(a, w)
        acc[:, span] = part if first else acc[:, span] + part
        at = at + w.shape[1]


def first_kernel(x, mem, gain, wq, wk, wv, q_ref, kv_ref, qkvm_ref, part_ref, *refs):
    bufs, (xs, ms, squares, acc, sems) = refs[:3], refs[3:]
    groups = []
    for k in range(D // KC):
        span = pl.ds(k * KC, KC)
        pairs = [(x.at[0, :, span], xs.at[:, span]), (mem.at[:, span], ms.at[:, span])]
        pairs += [(w.at[span, :], buf.at[span, :]) for w, buf in zip((wq, wk, wv), bufs)]
        groups.append(
            [pltpu.make_async_copy(p, q, sems.at[k, n]) for n, (p, q) in enumerate(pairs)]
        )
    for group in groups:
        for c in group:
            c.start()
    g = gain[...].astype(F32).reshape(1, D)
    for k, group in enumerate(groups):
        for c in group:
            c.wait()
        span = slice(k * KC, (k + 1) * KC)
        top = scaled_chunk(xs[:, span], g[:, span], squares, slice(0, ROWS), k == 0)
        low = scaled_chunk(ms[:, span], g[:, span], squares, slice(ROWS, ROWS + M), k == 0)
        a = jnp.concatenate([top, low], axis=0)
        accumulate(acc, a, [buf[span, :] for buf in bufs], k == 0)
    out = (acc[...] * norm_of(squares)).astype(BF)
    q_ref[...] = out[:ROWS, : 2 * HD]
    kv_ref[...] = out[:ROWS, 2 * HD :]
    qkvm_ref[...] = out[ROWS:, :]
    px, py, _, _ = place()
    memory_part(qkvm_ref[...], [kv_ref[...]], px + py == 0, part_ref)


def first_project(x, mem, gain, wq, wk, wv):
    hbm = pl.BlockSpec(memory_space=pltpu.HBM)
    shapes = [(ROWS, 2 * HD), (ROWS, 2 * HD), (M, 4 * HD), (2 * M, HD + 128)]
    shapes += [wq.shape, wk.shape, wv.shape]
    return pl.pallas_call(
        first_kernel,
        in_specs=[hbm, hbm, WHOLE, hbm, hbm, hbm],
        out_specs=[WHOLE] * len(shapes),
        out_shape=[jax.ShapeDtypeStruct(s, BF) for s in shapes],
        scratch_shapes=[
            pltpu.VMEM((ROWS, D), BF),
            pltpu.VMEM((M, D), BF),
            pltpu.VMEM((ROWS + M, 128), F32),
            pltpu.VMEM((ROWS + M, 4 * HD), F32),
            pltpu.SemaphoreType.DMA((D // KC, 5)),
        ],
        compiler_params=params(28),
        cost_estimate=pl.CostEstimate(
            flops=2 * (ROWS + M) * D * 4 * HD, bytes_accessed=10 * 2**20, transcendentals=512
        ),
        name="first_project",
    )(x, mem, gain, wq, wk, wv)


def window(h):
    return pl.multiple_of((h * 7 // 2) * 128, 128)


def second_kernel(x, gain, wq, wk, wv, q0, wt, proj, *refs):
    q_ref, kv_ref, wt_buf, proj_buf, cols_buf, xs, squares, acc, sems, wsems = refs
    _, _, z, c = place()
    copies = []
    for k in range(D // KC):
        span = pl.ds(k * KC, KC)
        copies.append(pltpu.make_async_copy(x.at[1, :, span], xs.at[:, span], sems.at[k]))
    late = [
        pltpu.make_async_copy(src, dst, wsems.at[n])
        for n, (src, dst) in enumerate(
            (
                (wt, wt_buf),
                (proj, proj_buf),
                (x.at[:, :, pl.ds(window(2 * z + c), 512)], cols_buf),
            )
        )
    ]
    for c in copies + late:
        c.start()
    q_ref[0] = q0[...]
    g = gain[...].astype(F32).reshape(1, D)
    for k, c in enumerate(copies):
        c.wait()
        span = slice(k * KC, (k + 1) * KC)
        a = scaled_chunk(xs[:, span], g[:, span], squares, slice(0, ROWS), k == 0)
        accumulate(acc, a, [w[span, :] for w in (wq, wk, wv)], k == 0)
    out = (acc[...] * norm_of(squares)).astype(BF)
    q_ref[1] = out[:, : 2 * HD]
    kv_ref[...] = out[:, 2 * HD :]
    for c in late:
        c.wait()


def second_project(x, gain, wq, wk, wv, q0, wt, proj):
    hbm = pl.BlockSpec(memory_space=pltpu.HBM)
    shapes = [(2, ROWS, 2 * HD), (ROWS, 2 * HD), wt.shape, proj.shape, (2, ROWS, 512)]
    return pl.pallas_call(
        second_kernel,
        in_specs=[hbm] + [WHOLE] * 5 + [hbm, hbm],
        out_specs=[WHOLE] * len(shapes),
        out_shape=[jax.ShapeDtypeStruct(s, BF) for s in shapes],
        scratch_shapes=[
            pltpu.VMEM((ROWS, D), BF),
            pltpu.VMEM((ROWS, 128), F32),
            pltpu.VMEM((ROWS, 4 * HD), F32),
            pltpu.SemaphoreType.DMA((D // KC,)),
            pltpu.SemaphoreType.DMA((3,)),
        ],
        compiler_params=params(28),
        cost_estimate=pl.CostEstimate(
            flops=2 * ROWS * D * 4 * HD, bytes_accessed=10 * 2**20, transcendentals=512
        ),
        name="second_project",
    )(x, gain, wq, wk, wv, q0, wt, proj)


def memory_project_kernel(own, other, gain, wq, wk, wv, *refs):
    kvs, (qkvm_ref, part_ref, whole_ref) = refs[:4], refs[4:]
    px, _, _, c = place()
    whole_ref[:, pl.ds(pl.multiple_of(c * HALF, 128), HALF)] = own[...]
    whole_ref[:, pl.ds(pl.multiple_of((1 - c) * HALF, 128), HALF)] = other[...]
    a = normed(whole_ref[...], gain[...].reshape(1, D))
    qkvm_ref[:, : 2 * HD] = dot(a, wq[...]).astype(BF)
    qkvm_ref[:, 2 * HD : 3 * HD] = dot(a, wk[...]).astype(BF)
    qkvm_ref[:, 3 * HD :] = dot(a, wv[...]).astype(BF)
    memory_part(qkvm_ref[...], [kv[...] for kv in kvs], px == 0, part_ref)


def memory_project(own, other, gain, wq, wk, wv, kvs):
    return pl.pallas_call(
        memory_project_kernel,
        in_specs=[WHOLE] * 10,
        out_specs=[WHOLE] * 3,
        out_shape=[
            jax.ShapeDtypeStruct((M, 4 * HD), BF),
            jax.ShapeDtypeStruct((2 * M, HD + 128), BF),
            jax.ShapeDtypeStruct((M, D), BF),
        ],
        compiler_params=params(20),
        cost_estimate=pl.CostEstimate(
            flops=2 * 256 * D * 4 * HD, bytes_accessed=8 * 1024 * 1024, transcendentals=M
        ),
        name="memory_project",
    )(own, other, gain, wq, wk, wv, *kvs)


def memory_combine_kernel(last, a, b, out_ref):
    parts = [r[...].astype(F32) for r in (a, b)]
    lses = [p[:, HD : HD + 1] + p[:, HD + 1 : HD + 2] for p in parts]
    peak = functools.reduce(jnp.maximum, lses)
    ws = [jnp.exp2(s - peak) for s in lses]
    total = sum(ws)
    out = sum(w * p[:, :HD] for w, p in zip(ws, parts)) / total
    if last:
        out_ref[:, :HD] = out[:M].astype(BF)
        out_ref[:, HD:] = out[M:].astype(BF)
    else:
        lse = peak + jnp.log2(total)
        hi = lse.astype(BF).astype(F32)
        lane = lax.broadcasted_iota(jnp.int32, (2 * M, 128), 1)
        stats = jnp.where(lane == 0, hi, jnp.where(lane == 1, lse - hi, 0.0))
        out_ref[:, :HD] = out.astype(BF)
        out_ref[:, HD:] = stats.astype(BF)


def memory_combine(a, b, last=False):
    shape = (M, 2 * HD) if last else (2 * M, HD + 128)
    return pl.pallas_call(
        functools.partial(memory_combine_kernel, last),
        in_specs=[WHOLE] * 2,
        out_specs=WHOLE,
        out_shape=jax.ShapeDtypeStruct(shape, BF),
        compiler_params=params(4),
        cost_estimate=pl.CostEstimate(flops=10**8, bytes_accessed=10**5, transcendentals=256),
        name="memory_combine",
    )(a, b)


def memory_write_kernel(blocks, mem, w_out, proj, keep_ref, send_ref):
    _, _, z, c = place()
    wide = mem[:, pl.ds(window(2 * z + c), 512)].astype(F32)
    acc = jnp.where(c == 1, wide[:, 64:], wide[:, :COLS])
    far = SHAPE - 1 - z
    for k, zz in enumerate((z, flip(z), far, flip(far))):
        for e in range(2):
            h = zz * 2 + (c if e == 0 else 1 - c)
            w = w_out[:, pl.ds(pl.multiple_of(h * 2 * HD, 2 * HD), 2 * HD)]
            acc = acc + dot_t(blocks[2 * k + e], w)
    a = acc.astype(BF)
    keep_ref[...] = dot(a, proj[:, pl.ds(pl.multiple_of(c * HALF, 128), HALF)]).astype(BF)
    send_ref[...] = dot(a, proj[:, pl.ds(pl.multiple_of((1 - c) * HALF, 128), HALF)]).astype(BF)


def finish_kernel(own, other, out_ref):
    _, _, _, c = place()
    out_ref[:, pl.ds(pl.multiple_of(c * HALF, 128), HALF)] = own[...]
    out_ref[:, pl.ds(pl.multiple_of((1 - c) * HALF, 128), HALF)] = other[...]


def finish(own, other):
    return pl.pallas_call(
        finish_kernel,
        in_specs=[WHOLE] * 2,
        out_specs=WHOLE,
        out_shape=jax.ShapeDtypeStruct((M, D), BF),
        compiler_params=params(4),
        name="finish",
    )(own, other)


def flip(i):
    return i + 1 - 2 * lax.rem(i, 2)


def memory_write(blocks, mem, w_out, proj):
    return pl.pallas_call(
        memory_write_kernel,
        in_specs=[WHOLE] * 4,
        out_specs=[WHOLE] * 2,
        out_shape=[jax.ShapeDtypeStruct((M, HALF), BF)] * 2,
        compiler_params=params(20),
        cost_estimate=pl.CostEstimate(
            flops=2 * 256 * D * 8 * COLS, bytes_accessed=8 * 1024 * 1024, transcendentals=0
        ),
        name="memory_write",
    )(blocks, mem, w_out, proj)


def token_kernel(seg, docs, q0, q1, q2, q3, kva, kvb, kvc, o0, o1, o2, o3, kvs, kcode):
    x, y, _, _ = place()
    lane = lax.broadcasted_iota(jnp.int32, (1, ROWS), 1).astype(F32)
    for n, ref in enumerate((kva, kvb, kvc)):
        kvs[n * ROWS : (n + 1) * ROWS, :] = ref[...]
        block = (y - 2 + n) * SHAPE + x
        start = jnp.maximum(block, 0) * ROWS
        doc = docs[seg : seg + 1, pl.ds(pl.multiple_of(start, ROWS), ROWS)].astype(F32)
        code = doc * 4096.0 + lane + start.astype(F32)
        kcode[:, n * ROWS : (n + 1) * ROWS] = jnp.where(block >= 0, code, -1.0)
    for d, (q_ref, o_ref) in enumerate(zip((q0, q1, q2, q3), (o0, o1, o2, o3))):
        start = (y * SHAPE + lax.rem(x - d + SHAPE, SHAPE)) * ROWS
        doc = docs[seg : seg + 1, pl.ds(pl.multiple_of(start, ROWS), ROWS)].astype(F32)
        low = column(doc * 4096.0)
        high = column(doc * 4096.0 + lane + start.astype(F32))
        if d == 0:
            codes = kcode[...]
            keys = kvs[...]
        else:
            at = jnp.where(x >= d, 0, ROWS)
            at = pl.multiple_of(at, ROWS)
            codes = kcode[:, pl.ds(at, 2 * ROWS)]
            keys = kvs[pl.ds(at, 2 * ROWS), :]
        valid = (codes >= low) & (codes <= high)
        for g in range(2):
            q = q_ref[seg, :, g * HD : (g + 1) * HD]
            scores = jnp.where(valid, dot_t(q, keys[:, :HD]) * LOG2E_SCALE, LOW)
            out, lse = attend([scores], [keys[:, HD:]])
            row = as_row(lse)
            hi = row.astype(BF).astype(F32)
            sub = lax.broadcasted_iota(jnp.int32, (16, ROWS), 0)
            stats = jnp.where(sub == 0, hi, jnp.where(sub == 1, row - hi, 0.0))
            o_ref[:ROWS, g * HD : (g + 1) * HD] = out.astype(BF)
            o_ref[ROWS:, g * HD : (g + 1) * HD] = stats.astype(BF)


def token_attention(docs, seg, qs, kva, kvb, kvc):
    return pl.pallas_call(
        functools.partial(token_kernel, seg),
        in_specs=[WHOLE] * 8,
        out_specs=[WHOLE] * 4,
        out_shape=[jax.ShapeDtypeStruct((ROWS + 16, 2 * HD), BF)] * 4,
        scratch_shapes=[pltpu.VMEM((3 * ROWS, 2 * HD), BF), pltpu.VMEM((1, 3 * ROWS), F32)],
        compiler_params=params(16),
        cost_estimate=pl.CostEstimate(
            flops=3 * 10**9, bytes_accessed=4 * 10**6, transcendentals=10**6
        ),
        name="token_attention",
    )(docs, *qs, kva, kvb, kvc)


def token_combine_kernel(seg, q, qkvm, a, b, c, d, out_ref):
    refs = (a, b, c, d)
    for g in range(2):
        lanes = slice(g * HD, (g + 1) * HD)
        scores = dot_t(q[seg, :, lanes], qkvm[:, 2 * HD : 3 * HD]) * LOG2E_SCALE
        out, lse = attend([scores], [qkvm[:, 3 * HD :]])
        outs, lses = [out], [lse]
        for r in refs:
            tail = r[ROWS:, lanes].astype(F32)
            lses.append(column(tail[0:1, :] + tail[1:2, :]))
            outs.append(r[:ROWS, lanes].astype(F32))
        peak = functools.reduce(jnp.maximum, lses)
        ws = [jnp.exp2(s - peak) for s in lses]
        mixed = sum(w * o for w, o in zip(ws, outs)) / sum(ws)
        out_ref[:, lanes] = mixed.astype(BF)


def token_combine(seg, q, qkvm, parts):
    return pl.pallas_call(
        functools.partial(token_combine_kernel, seg),
        in_specs=[WHOLE] * 6,
        out_specs=WHOLE,
        out_shape=jax.ShapeDtypeStruct((ROWS, 2 * HD), BF),
        compiler_params=params(12),
        cost_estimate=pl.CostEstimate(flops=5 * 10**8, bytes_accessed=10**6, transcendentals=4096),
        name="token_combine",
    )(q, qkvm, *parts)


def token_out_kernel(seg, *refs):
    blocks, cols, w_out, out_ref, flat = refs[:8], refs[8], refs[9], refs[-2], refs[-1]
    _, _, z, c = place()
    acc = jnp.zeros((COLS, ROWS), F32)
    for n, ref in enumerate(blocks):
        k, e = n // 2, n % 2
        h = lax.rem(z - k + SHAPE, SHAPE) * 2 + (c if e == 0 else 1 - c)
        w = w_out[:, pl.ds(pl.multiple_of(h * 2 * HD, 2 * HD), 2 * HD)]
        acc = acc + dot_t(w, ref[...])
    for at in range(0, 512, 128):
        flat[at : at + 128, :] = cols[seg, :, at : at + 128].astype(F32).T
    out_ref[0] = (acc + flat[pl.ds(pl.multiple_of(c * 64, 64), COLS), :]).astype(BF)


def token_out(blocks, cols, seg, w_out, before):
    in_specs = [WHOLE] * 10
    args = [*blocks, cols, w_out]
    aliases = {}
    if before is not None:
        in_specs.append(pl.BlockSpec(memory_space=pl.ANY))
        args.append(before)
        aliases = {len(args) - 1: 0}
    return pl.pallas_call(
        functools.partial(token_out_kernel, seg),
        grid=(1,),
        in_specs=in_specs,
        out_specs=pl.BlockSpec((1, COLS, ROWS), lambda k: (seg, 0, 0)),
        out_shape=jax.ShapeDtypeStruct((2, COLS, ROWS), BF),
        input_output_aliases=aliases,
        scratch_shapes=[pltpu.VMEM((512, ROWS), F32)],
        compiler_params=params(12),
        cost_estimate=pl.CostEstimate(
            flops=2 * ROWS * 4096 * COLS, bytes_accessed=6 * 10**6, transcendentals=0
        ),
        name="token_out",
    )(*args)


N_SEQ, N_HEAD = SHAPE * SHAPE, 8


def x_shift(v, d):
    return lax.ppermute(
        v, "seq", [(i, i // SHAPE * SHAPE + (i + d) % SHAPE) for i in range(N_SEQ)]
    )


def y_shift(v, d):
    return lax.ppermute(v, "seq", [(i, (i + d * SHAPE) % N_SEQ) for i in range(N_SEQ)])


def y_later(v, d):
    return lax.ppermute(v, "seq", [(i, i + d * SHAPE) for i in range(N_SEQ - d * SHAPE)])


def x_near(v):
    return lax.ppermute(v, "seq", [(i, i ^ 1) for i in range(N_SEQ)])


def x_far(v):
    return lax.ppermute(v, "seq", [(i, i ^ 3) for i in range(N_SEQ)])


def y_near(v):
    return lax.ppermute(v, "seq", [(i, i ^ 4) for i in range(N_SEQ)])


def y_far(v):
    return lax.ppermute(v, "seq", [(i, i ^ 12) for i in range(N_SEQ)])


def z_near(v):
    return lax.ppermute(v, "head", [(i, i ^ 2) for i in range(N_HEAD)])


def z_far(v):
    return lax.ppermute(v, "head", [(i, i ^ 6) for i in range(N_HEAD)])


def z_shift(v, d):
    return lax.ppermute(v, "head", [(i, (i + 2 * d) % N_HEAD) for i in range(N_HEAD)])


def other_core(v):
    return lax.ppermute(v, "head", [(i, i ^ 1) for i in range(N_HEAD)])


def add(a, b):
    return (a.astype(F32) + b.astype(F32)).astype(BF)


def memory_tail(attn, mem, w_out, proj):
    pair = jnp.stack([attn, other_core(attn)])
    four = jnp.concatenate([pair, z_near(pair)])
    blocks = jnp.concatenate([four, z_far(four)])
    keep, send = memory_write(blocks, mem, w_out, proj)
    half = add(keep, other_core(send))
    half = add(half, z_near(half))
    half = add(half, z_far(half))
    return half, other_core(half)


def per_device(segment_input, doc_ids, memory, gain, w_query, w_key, w_value, w_out, mem_proj):
    in_hbm = lambda v: pltpu.with_memory_space_constraint(v, pltpu.HBM)
    x = in_hbm(segment_input)

    q0, kv0, qkvm0, part, *weights = first_project(
        x, in_hbm(memory), gain, *[in_hbm(w) for w in (w_query, w_key, w_value)]
    )
    weights = (gain, *weights)
    q, kv1, w_out, mem_proj, cols = second_project(
        x, *weights, q0, in_hbm(w_out.T), in_hbm(mem_proj)
    )

    part = memory_combine(part, x_near(part))
    part = memory_combine(part, x_far(part))
    part = memory_combine(part, y_near(part))
    attn = memory_combine(part, y_far(part), True)
    own, other = memory_tail(attn, memory, w_out, mem_proj)

    kvs0 = [kv0] + [y_later(kv0, d) for d in (1, 2)]
    kvs1 = [kv1] + [y_shift(kv1, d) for d in (1, 2, 3)]
    qkvm1, part, mem1 = memory_project(own, other, *weights, kvs1)
    part = memory_combine(part, x_near(part))
    attn = memory_combine(part, x_far(part), True)
    own, other = memory_tail(attn, mem1, w_out, mem_proj)

    hidden = None
    qs = [q] + [x_shift(q, d) for d in (1, 2, 3)]
    for s, (kvs, qkvm) in enumerate(((kvs0, qkvm0), (kvs1, qkvm1))):
        parts = token_attention(doc_ids, s, qs, kvs[2], kvs[1], kvs[0])
        parts = [parts[0]] + [x_shift(parts[d], SHAPE - d) for d in (1, 2, 3)]
        attn = token_combine(s, q, qkvm, parts)
        blocks = []
        for d in range(SHAPE):
            piece = attn if d == 0 else z_shift(attn, d)
            blocks += [piece, other_core(piece)]
        hidden = token_out(blocks, cols, s, w_out, hidden)

    return hidden.transpose(0, 2, 1), finish(own, other)


def solution(mesh):
    return jax.shard_map(
        per_device,
        mesh=mesh,
        in_specs=(
            P(None, "seq", None),
            P(),
            P(),
            P(),
            P(None, "head"),
            P(None, "head"),
            P(None, "head"),
            P(None, "head"),
            P("head", None),
        ),
        out_specs=(P(None, "seq", "head"), P()),
        check_vma=False,
    )
```

```python
import functools
import math

import jax
import jax.numpy as jnp
from jax import lax
from jax.experimental import pallas as pl
from jax.experimental.pallas import tpu as pltpu
from jax.sharding import PartitionSpec as P


D = 3584
HD = 256
M = 32
ROWS = 256
COLS = 448
HALF = D // 2
KC = 512
SHAPE = 4
LOG2E_SCALE = math.log2(math.e) / 16.0
LOW = -1e30
BF = jnp.bfloat16
F32 = jnp.float32


WHOLE = pl.BlockSpec(memory_space=pltpu.VMEM)


def params(mib, **kw):
    return pltpu.CompilerParams(vmem_limit_bytes=mib * 1024 * 1024, **kw)


def dot(a, b):
    return jnp.dot(a, b, preferred_element_type=F32)


def dot_t(a, b):
    return lax.dot_general(a, b, (((1,), (1,)), ((), ())), preferred_element_type=F32)


def normed(rows, gain):
    v = rows.astype(F32)
    r = lax.rsqrt(jnp.mean(v * v, axis=-1, keepdims=True) + 1e-6)
    return (v * r * gain.astype(F32)).astype(BF)


def column(row):
    return jnp.broadcast_to(row, (128, row.shape[1])).T[:, :1]


def as_row(col):
    return jnp.broadcast_to(col, (col.shape[0], 128)).T[:1, :]


def attend(score_list, value_list):
    peak = functools.reduce(jnp.maximum, [jnp.max(s, axis=1, keepdims=True) for s in score_list])
    peak = jnp.maximum(peak, -1e29)
    total = 0.0
    mixed = 0.0
    for s, v in zip(score_list, value_list):
        p = jnp.exp2(s - peak)
        total = total + jnp.sum(p, axis=1, keepdims=True)
        mixed = mixed + dot(p.astype(BF), v)
    some = total > 0.0
    out = mixed / jnp.where(some, total, 1.0)
    return out, jnp.where(some, peak + jnp.log2(jnp.where(some, total, 1.0)), LOW)


def memory_part(qkvm, key_blocks, first, out_ref):
    for g in range(2):
        q = qkvm[:, g * HD : (g + 1) * HD]
        scores = [dot_t(q, kv[:, :HD]) * LOG2E_SCALE for kv in key_blocks]
        sm = dot_t(q, qkvm[:, 2 * HD : 3 * HD]) * LOG2E_SCALE
        scores.append(jnp.where(first, sm, LOW))
        out, lse = attend(scores, [kv[:, HD:] for kv in key_blocks] + [qkvm[:, 3 * HD :]])
        hi = lse.astype(BF)
        lo = (lse - hi.astype(F32)).astype(BF)
        lane = lax.broadcasted_iota(jnp.int32, (M, 128), 1)
        stats = jnp.where(lane == 0, hi.astype(F32), jnp.where(lane == 1, lo.astype(F32), 0.0))
        out_ref[g * M : (g + 1) * M, :HD] = out.astype(BF)
        out_ref[g * M : (g + 1) * M, HD:] = stats.astype(BF)


def place():
    i = lax.axis_index("seq")
    h = lax.axis_index("head")
    return i % SHAPE, i // SHAPE, h // 2, h % 2


def scaled_chunk(x, gain, squares, rows, first):
    v = x.astype(F32)
    sq = v * v
    part = sq[:, :128]
    for n in range(1, KC // 128):
        part = part + sq[:, n * 128 : (n + 1) * 128]
    squares[rows, :] = part if first else squares[rows, :] + part
    return (v * gain).astype(BF)


def norm_of(squares):
    return lax.rsqrt(jnp.sum(squares[...], axis=1, keepdims=True) / D + 1e-6)


def accumulate(acc, a, ws, first):
    at = 0
    for w in ws:
        span = slice(at, at + w.shape[1])
        part = dot(a, w)
        acc[:, span] = part if first else acc[:, span] + part
        at = at + w.shape[1]


def first_kernel(x, mem, gain, wq, wk, wv, q_ref, kv_ref, qkvm_ref, part_ref, *refs):
    bufs, (xs, ms, squares, acc, sems) = refs[:3], refs[3:]
    groups = []
    for k in range(D // KC):
        span = pl.ds(k * KC, KC)
        pairs = [(x.at[0, :, span], xs.at[:, span]), (mem.at[:, span], ms.at[:, span])]
        pairs += [(w.at[span, :], buf.at[span, :]) for w, buf in zip((wq, wk, wv), bufs)]
        groups.append(
            [pltpu.make_async_copy(p, q, sems.at[k, n]) for n, (p, q) in enumerate(pairs)]
        )
    for group in groups:
        for c in group:
            c.start()
    g = gain[...].astype(F32).reshape(1, D)
    for k, group in enumerate(groups):
        for c in group:
            c.wait()
        span = slice(k * KC, (k + 1) * KC)
        top = scaled_chunk(xs[:, span], g[:, span], squares, slice(0, ROWS), k == 0)
        low = scaled_chunk(ms[:, span], g[:, span], squares, slice(ROWS, ROWS + M), k == 0)
        a = jnp.concatenate([top, low], axis=0)
        accumulate(acc, a, [buf[span, :] for buf in bufs], k == 0)
    out = (acc[...] * norm_of(squares)).astype(BF)
    q_ref[...] = out[:ROWS, : 2 * HD]
    kv_ref[...] = out[:ROWS, 2 * HD :]
    qkvm_ref[...] = out[ROWS:, :]
    px, py, _, _ = place()
    memory_part(qkvm_ref[...], [kv_ref[...]], px + py == 0, part_ref)


def first_project(x, mem, gain, wq, wk, wv):
    hbm = pl.BlockSpec(memory_space=pltpu.HBM)
    shapes = [(ROWS, 2 * HD), (ROWS, 2 * HD), (M, 4 * HD), (2 * M, HD + 128)]
    shapes += [wq.shape, wk.shape, wv.shape]
    return pl.pallas_call(
        first_kernel,
        in_specs=[hbm, hbm, WHOLE, hbm, hbm, hbm],
        out_specs=[WHOLE] * len(shapes),
        out_shape=[jax.ShapeDtypeStruct(s, BF) for s in shapes],
        scratch_shapes=[
            pltpu.VMEM((ROWS, D), BF),
            pltpu.VMEM((M, D), BF),
            pltpu.VMEM((ROWS + M, 128), F32),
            pltpu.VMEM((ROWS + M, 4 * HD), F32),
            pltpu.SemaphoreType.DMA((D // KC, 5)),
        ],
        compiler_params=params(28),
        cost_estimate=pl.CostEstimate(
            flops=2 * (ROWS + M) * D * 4 * HD, bytes_accessed=10 * 2**20, transcendentals=512
        ),
        name="first_project",
    )(x, mem, gain, wq, wk, wv)


def window(h):
    return pl.multiple_of((h * 7 // 2) * 128, 128)


def second_kernel(x, gain, wq, wk, wv, wt, proj, *refs):
    q_ref, kv_ref, wt_buf, proj_buf, cols_buf, xs, squares, acc, sems, wsems = refs
    _, _, z, c = place()
    copies = []
    for k in range(D // KC):
        span = pl.ds(k * KC, KC)
        copies.append(pltpu.make_async_copy(x.at[1, :, span], xs.at[:, span], sems.at[k]))
    late = [
        pltpu.make_async_copy(src, dst, wsems.at[n])
        for n, (src, dst) in enumerate(
            (
                (wt, wt_buf),
                (proj, proj_buf),
                (x.at[:, :, pl.ds(window(2 * z + c), 512)], cols_buf),
            )
        )
    ]
    for c in copies + late:
        c.start()
    g = gain[...].astype(F32).reshape(1, D)
    for k, c in enumerate(copies):
        c.wait()
        span = slice(k * KC, (k + 1) * KC)
        a = scaled_chunk(xs[:, span], g[:, span], squares, slice(0, ROWS), k == 0)
        accumulate(acc, a, [w[span, :] for w in (wq, wk, wv)], k == 0)
    out = (acc[...] * norm_of(squares)).astype(BF)
    q_ref[...] = out[:, : 2 * HD]
    kv_ref[...] = out[:, 2 * HD :]
    for c in late:
        c.wait()


def second_project(x, gain, wq, wk, wv, wt, proj):
    hbm = pl.BlockSpec(memory_space=pltpu.HBM)
    shapes = [(ROWS, 2 * HD), (ROWS, 2 * HD), wt.shape, proj.shape, (2, ROWS, 512)]
    return pl.pallas_call(
        second_kernel,
        in_specs=[hbm] + [WHOLE] * 4 + [hbm, hbm],
        out_specs=[WHOLE] * len(shapes),
        out_shape=[jax.ShapeDtypeStruct(s, BF) for s in shapes],
        scratch_shapes=[
            pltpu.VMEM((ROWS, D), BF),
            pltpu.VMEM((ROWS, 128), F32),
            pltpu.VMEM((ROWS, 4 * HD), F32),
            pltpu.SemaphoreType.DMA((D // KC,)),
            pltpu.SemaphoreType.DMA((3,)),
        ],
        compiler_params=params(28),
        cost_estimate=pl.CostEstimate(
            flops=2 * ROWS * D * 4 * HD, bytes_accessed=10 * 2**20, transcendentals=512
        ),
        name="second_project",
    )(x, gain, wq, wk, wv, wt, proj)


def memory_project_kernel(own, other, gain, wq, wk, wv, *refs):
    kvs, (qkvm_ref, part_ref, whole_ref) = refs[:4], refs[4:]
    px, _, _, c = place()
    whole_ref[:, pl.ds(pl.multiple_of(c * HALF, 128), HALF)] = own[...]
    whole_ref[:, pl.ds(pl.multiple_of((1 - c) * HALF, 128), HALF)] = other[...]
    a = normed(whole_ref[...], gain[...].reshape(1, D))
    qkvm_ref[:, : 2 * HD] = dot(a, wq[...]).astype(BF)
    qkvm_ref[:, 2 * HD : 3 * HD] = dot(a, wk[...]).astype(BF)
    qkvm_ref[:, 3 * HD :] = dot(a, wv[...]).astype(BF)
    memory_part(qkvm_ref[...], [kv[...] for kv in kvs], px == 0, part_ref)


def memory_project(own, other, gain, wq, wk, wv, kvs):
    return pl.pallas_call(
        memory_project_kernel,
        in_specs=[WHOLE] * 10,
        out_specs=[WHOLE] * 3,
        out_shape=[
            jax.ShapeDtypeStruct((M, 4 * HD), BF),
            jax.ShapeDtypeStruct((2 * M, HD + 128), BF),
            jax.ShapeDtypeStruct((M, D), BF),
        ],
        compiler_params=params(20),
        cost_estimate=pl.CostEstimate(
            flops=2 * 256 * D * 4 * HD, bytes_accessed=8 * 1024 * 1024, transcendentals=M
        ),
        name="memory_project",
    )(own, other, gain, wq, wk, wv, *kvs)


def memory_combine_kernel(last, a, b, out_ref):
    parts = [r[...].astype(F32) for r in (a, b)]
    lses = [p[:, HD : HD + 1] + p[:, HD + 1 : HD + 2] for p in parts]
    peak = functools.reduce(jnp.maximum, lses)
    ws = [jnp.exp2(s - peak) for s in lses]
    total = sum(ws)
    out = sum(w * p[:, :HD] for w, p in zip(ws, parts)) / total
    if last:
        out_ref[:, :HD] = out[:M].astype(BF)
        out_ref[:, HD:] = out[M:].astype(BF)
    else:
        lse = peak + jnp.log2(total)
        hi = lse.astype(BF).astype(F32)
        lane = lax.broadcasted_iota(jnp.int32, (2 * M, 128), 1)
        stats = jnp.where(lane == 0, hi, jnp.where(lane == 1, lse - hi, 0.0))
        out_ref[:, :HD] = out.astype(BF)
        out_ref[:, HD:] = stats.astype(BF)


def memory_combine(a, b, last=False):
    shape = (M, 2 * HD) if last else (2 * M, HD + 128)
    return pl.pallas_call(
        functools.partial(memory_combine_kernel, last),
        in_specs=[WHOLE] * 2,
        out_specs=WHOLE,
        out_shape=jax.ShapeDtypeStruct(shape, BF),
        compiler_params=params(4),
        cost_estimate=pl.CostEstimate(flops=10**8, bytes_accessed=10**5, transcendentals=256),
        name="memory_combine",
    )(a, b)


def pair_kernel(a, b, out_ref):
    out_ref[0] = a[...]
    out_ref[1] = b[...]


def pair_up(a, b):
    return pl.pallas_call(
        pair_kernel,
        in_specs=[WHOLE] * 2,
        out_specs=WHOLE,
        out_shape=jax.ShapeDtypeStruct((2, *a.shape), BF),
        compiler_params=params(4),
        name="pair_up",
    )(a, b)


def gathered_heads():
    _, _, z, c = place()
    side = 1 - 2 * c
    before, after = lax.rem(z - side + SHAPE, SHAPE), lax.rem(z + side + SHAPE, SHAPE)
    far = lax.rem(z + 2, SHAPE)
    chips = (z, z, before, before, after, after, far, far)
    cores = (c, 1 - c, c, 1 - c, 1 - c, c, c, 1 - c)
    return [2 * zz + cc for zz, cc in zip(chips, cores)]


def block_values(refs):
    own, swapped, near, near2, far = refs[:5]
    last = [far[0], far[1]] if len(refs) == 5 else [far[...], refs[5][...]]
    return [own[...], swapped[...], near[0], near[1], near2[0], near2[1], *last]


def memory_write_kernel(o, o2, n, n2, f, f2, mem, w_out, proj, keep_ref, send_ref):
    _, _, z, c = place()
    wide = mem[:, pl.ds(window(2 * z + c), 512)].astype(F32)
    acc = jnp.where(c == 1, wide[:, 64:], wide[:, :COLS])
    for h, v in zip(gathered_heads(), block_values((o, o2, n, n2, f, f2))):
        acc = acc + dot_t(v, w_out[:, pl.ds(pl.multiple_of(h * 2 * HD, 2 * HD), 2 * HD)])
    a = acc.astype(BF)
    keep_ref[...] = dot(a, proj[:, pl.ds(pl.multiple_of(c * HALF, 128), HALF)]).astype(BF)
    send_ref[...] = dot(a, proj[:, pl.ds(pl.multiple_of((1 - c) * HALF, 128), HALF)]).astype(BF)


def finish_kernel(own, other, out_ref):
    _, _, _, c = place()
    out_ref[:, pl.ds(pl.multiple_of(c * HALF, 128), HALF)] = own[...]
    out_ref[:, pl.ds(pl.multiple_of((1 - c) * HALF, 128), HALF)] = other[...]


def finish(own, other):
    return pl.pallas_call(
        finish_kernel,
        in_specs=[WHOLE] * 2,
        out_specs=WHOLE,
        out_shape=jax.ShapeDtypeStruct((M, D), BF),
        compiler_params=params(4),
        name="finish",
    )(own, other)


def memory_write(blocks, mem, w_out, proj):
    return pl.pallas_call(
        memory_write_kernel,
        in_specs=[WHOLE] * 9,
        out_specs=[WHOLE] * 2,
        out_shape=[jax.ShapeDtypeStruct((M, HALF), BF)] * 2,
        compiler_params=params(20),
        cost_estimate=pl.CostEstimate(
            flops=2 * 256 * D * 8 * COLS, bytes_accessed=8 * 1024 * 1024, transcendentals=0
        ),
        name="memory_write",
    )(*blocks, mem, w_out, proj)


def token_kernel(seg, docs, q0, q1, q2, q3, kva, kvb, kvb2, kvc, o0, o1, o2, o3, kvs, kcode):
    x, y, _, _ = place()
    lane = lax.broadcasted_iota(jnp.int32, (1, ROWS), 1).astype(F32)
    for n, ref in enumerate((kva, kvb, kvc)):
        if n == 1:
            kvs[ROWS : 2 * ROWS, :] = jnp.where(y % 2 == 1, kvb[...], kvb2[...])
        else:
            kvs[n * ROWS : (n + 1) * ROWS, :] = ref[...]
        block = (y - 2 + n) * SHAPE + x
        start = jnp.maximum(block, 0) * ROWS
        doc = docs[seg : seg + 1, pl.ds(pl.multiple_of(start, ROWS), ROWS)].astype(F32)
        code = doc * 4096.0 + lane + start.astype(F32)
        kcode[:, n * ROWS : (n + 1) * ROWS] = jnp.where(block >= 0, code, -1.0)
    for d, (q_ref, o_ref) in enumerate(zip((q0, q1, q2, q3), (o0, o1, o2, o3))):
        start = (y * SHAPE + lax.bitwise_xor(x, d)) * ROWS
        doc = docs[seg : seg + 1, pl.ds(pl.multiple_of(start, ROWS), ROWS)].astype(F32)
        low = column(doc * 4096.0)
        high = column(doc * 4096.0 + lane + start.astype(F32))
        if d == 0:
            codes = kcode[...]
            keys = kvs[...]
        else:
            at = jnp.where(lax.bitwise_xor(x, d) < x, 0, ROWS)
            at = pl.multiple_of(at, ROWS)
            codes = kcode[:, pl.ds(at, 2 * ROWS)]
            keys = kvs[pl.ds(at, 2 * ROWS), :]
        valid = (codes >= low) & (codes <= high)
        for g in range(2):
            q = q_ref[:, g * HD : (g + 1) * HD]
            scores = jnp.where(valid, dot_t(q, keys[:, :HD]) * LOG2E_SCALE, LOW)
            out, lse = attend([scores], [keys[:, HD:]])
            row = as_row(lse)
            hi = row.astype(BF).astype(F32)
            sub = lax.broadcasted_iota(jnp.int32, (16, ROWS), 0)
            stats = jnp.where(sub == 0, hi, jnp.where(sub == 1, row - hi, 0.0))
            o_ref[:ROWS, g * HD : (g + 1) * HD] = out.astype(BF)
            o_ref[ROWS:, g * HD : (g + 1) * HD] = stats.astype(BF)


def token_attention(docs, seg, qs, kva, kvb, kvb2, kvc):
    return pl.pallas_call(
        functools.partial(token_kernel, seg),
        in_specs=[WHOLE] * 9,
        out_specs=[WHOLE] * 4,
        out_shape=[jax.ShapeDtypeStruct((ROWS + 16, 2 * HD), BF)] * 4,
        scratch_shapes=[pltpu.VMEM((3 * ROWS, 2 * HD), BF), pltpu.VMEM((1, 3 * ROWS), F32)],
        compiler_params=params(16),
        cost_estimate=pl.CostEstimate(
            flops=3 * 10**9, bytes_accessed=4 * 10**6, transcendentals=10**6
        ),
        name="token_attention",
    )(docs, *qs, kva, kvb, kvb2, kvc)


def token_combine_kernel(q, qkvm, a, b, c, d, out_ref):
    refs = (a, b, c, d)
    for g in range(2):
        lanes = slice(g * HD, (g + 1) * HD)
        scores = dot_t(q[:, lanes], qkvm[:, 2 * HD : 3 * HD]) * LOG2E_SCALE
        out, lse = attend([scores], [qkvm[:, 3 * HD :]])
        outs, lses = [out], [lse]
        for r in refs:
            tail = r[ROWS:, lanes].astype(F32)
            lses.append(column(tail[0:1, :] + tail[1:2, :]))
            outs.append(r[:ROWS, lanes].astype(F32))
        peak = functools.reduce(jnp.maximum, lses)
        ws = [jnp.exp2(s - peak) for s in lses]
        mixed = sum(w * o for w, o in zip(ws, outs)) / sum(ws)
        out_ref[:, lanes] = mixed.astype(BF)


def token_combine(q, qkvm, parts):
    return pl.pallas_call(
        token_combine_kernel,
        in_specs=[WHOLE] * 6,
        out_specs=WHOLE,
        out_shape=jax.ShapeDtypeStruct((ROWS, 2 * HD), BF),
        compiler_params=params(12),
        cost_estimate=pl.CostEstimate(flops=5 * 10**8, bytes_accessed=10**6, transcendentals=4096),
        name="token_combine",
    )(q, qkvm, *parts)


def token_out_kernel(seg, *refs):
    blocks, cols, w_out, out_ref, flat = refs[:5], *refs[5:]
    acc = features(cols, seg, flat)
    for h, v in zip(gathered_heads(), block_values(blocks)):
        acc = acc + dot_t(w_out[:, pl.ds(pl.multiple_of(h * 2 * HD, 2 * HD), 2 * HD)], v)
    out_ref[0] = acc.astype(BF)


def features(cols, seg, flat):
    _, _, _, c = place()
    for at in range(0, 512, 128):
        flat[at : at + 128, :] = cols[seg, :, at : at + 128].astype(F32).T
    return flat[pl.ds(pl.multiple_of(c * 64, 64), COLS), :]


def token_out(blocks, cols, seg, w_out):
    return pl.pallas_call(
        functools.partial(token_out_kernel, seg),
        grid=(1,),
        in_specs=[WHOLE] * 7,
        out_specs=pl.BlockSpec((1, COLS, ROWS), lambda k: (seg, 0, 0)),
        out_shape=jax.ShapeDtypeStruct((2, COLS, ROWS), BF),
        scratch_shapes=[pltpu.VMEM((512, ROWS), F32)],
        compiler_params=params(12),
        cost_estimate=pl.CostEstimate(
            flops=2 * ROWS * 4096 * COLS, bytes_accessed=6 * 10**6, transcendentals=0
        ),
        name="token_out",
    )(*blocks, cols, w_out)


def early_kernel(seg, *refs):
    cols, w_out, out_ref, flat = refs[4:]
    own, swapped, near, near2 = refs[:4]
    values = [own[...], swapped[...], near[0], near[1], near2[0], near2[1]]
    acc = features(cols, seg, flat)
    for h, v in zip(gathered_heads(), values):
        acc = acc + dot_t(w_out[:, pl.ds(pl.multiple_of(h * 2 * HD, 2 * HD), 2 * HD)], v)
    out_ref[...] = acc


def token_out_early(blocks, cols, seg, w_out):
    return pl.pallas_call(
        functools.partial(early_kernel, seg),
        in_specs=[WHOLE] * 6,
        out_specs=WHOLE,
        out_shape=jax.ShapeDtypeStruct((COLS, ROWS), F32),
        scratch_shapes=[pltpu.VMEM((512, ROWS), F32)],
        compiler_params=params(12),
        cost_estimate=pl.CostEstimate(
            flops=2 * ROWS * 3072 * COLS, bytes_accessed=5 * 10**6, transcendentals=0
        ),
        name="token_out_early",
    )(*blocks, cols, w_out)


def late_kernel(far, early, w_out, before, out_ref):
    acc = early[...]
    for h, v in zip(gathered_heads()[6:], (far[0], far[1])):
        acc = acc + dot_t(w_out[:, pl.ds(pl.multiple_of(h * 2 * HD, 2 * HD), 2 * HD)], v)
    out_ref[0] = acc.astype(BF)


def token_out_late(far, early, seg, w_out, before):
    return pl.pallas_call(
        late_kernel,
        grid=(1,),
        in_specs=[WHOLE] * 3 + [pl.BlockSpec(memory_space=pl.ANY)],
        out_specs=pl.BlockSpec((1, COLS, ROWS), lambda k: (seg, 0, 0)),
        out_shape=jax.ShapeDtypeStruct((2, COLS, ROWS), BF),
        input_output_aliases={3: 0},
        compiler_params=params(12),
        cost_estimate=pl.CostEstimate(
            flops=2 * ROWS * 1024 * COLS, bytes_accessed=3 * 10**6, transcendentals=0
        ),
        name="token_out_late",
    )(far, early, w_out, before)


N_SEQ, N_HEAD = SHAPE * SHAPE, 8


def x_xor(v, d):
    return lax.ppermute(v, "seq", [(i, i ^ d) for i in range(N_SEQ)])


def y_xor(v, d):
    return x_xor(v, 4 * d)


def y_later(v):
    return lax.ppermute(v, "seq", [(i, i + SHAPE) for i in range(N_SEQ - SHAPE)])


def all_four(send, v):
    near = send(v, 1)
    return [v, near, send(near, 3), send(v, 3)]


def x_near(v):
    return lax.ppermute(v, "seq", [(i, i ^ 1) for i in range(N_SEQ)])


def x_far(v):
    return lax.ppermute(v, "seq", [(i, i ^ 3) for i in range(N_SEQ)])


def y_near(v):
    return lax.ppermute(v, "seq", [(i, i ^ 4) for i in range(N_SEQ)])


def y_far(v):
    return lax.ppermute(v, "seq", [(i, i ^ 12) for i in range(N_SEQ)])


def z_near(v):
    return lax.ppermute(v, "head", [(i, i ^ 2) for i in range(N_HEAD)])


def z_far(v):
    return lax.ppermute(v, "head", [(i, i ^ 6) for i in range(N_HEAD)])


def z_turn(v):
    return lax.ppermute(v, "head", [(i, (i + 2 - 4 * (i % 2)) % N_HEAD) for i in range(N_HEAD)])


def z_two(v):
    return lax.ppermute(v, "head", [(i, (i + 4) % N_HEAD) for i in range(N_HEAD)])


def other_core(v):
    return lax.ppermute(v, "head", [(i, i ^ 1) for i in range(N_HEAD)])


def add(a, b):
    return (a.astype(F32) + b.astype(F32)).astype(BF)


def gather_heads(v):
    far = z_two(v)
    swapped = other_core(v)
    near = z_turn(pair_up(v, swapped))
    near2 = other_core(near)
    return v, swapped, near, near2, far, other_core(far)


def gather_heads_relay(v):
    swapped = other_core(v)
    near = z_turn(pair_up(v, swapped))
    far = z_turn(near)
    return v, swapped, near, other_core(near), far


def memory_tail(attn, mem, w_out, proj):
    blocks = gather_heads(attn)
    keep, send = memory_write(blocks, mem, w_out, proj)
    half = add(keep, other_core(send))
    half = add(half, z_near(half))
    half = add(half, z_far(half))
    return half, other_core(half)


def per_device(segment_input, doc_ids, memory, gain, w_query, w_key, w_value, w_out, mem_proj):
    in_hbm = lambda v: pltpu.with_memory_space_constraint(v, pltpu.HBM)
    x = in_hbm(segment_input)

    q0, kv0, qkvm0, part, *weights = first_project(
        x, in_hbm(memory), gain, *[in_hbm(w) for w in (w_query, w_key, w_value)]
    )
    weights = (gain, *weights)
    q1, kv1, w_out, mem_proj, cols = second_project(x, *weights, in_hbm(w_out.T), in_hbm(mem_proj))

    part = memory_combine(part, x_near(part))
    part = memory_combine(part, x_far(part))
    part = memory_combine(part, y_near(part))
    attn = memory_combine(part, y_far(part), True)
    own, other = memory_tail(attn, memory, w_out, mem_proj)

    next_row = y_later(kv0)
    kvs0 = [kv0, next_row, y_later(next_row), next_row]
    kvs1 = all_four(y_xor, kv1)
    qkvm1, part, mem1 = memory_project(own, other, *weights, kvs1)
    part = memory_combine(part, x_near(part))
    attn = memory_combine(part, x_far(part), True)
    own, other = memory_tail(attn, mem1, w_out, mem_proj)

    for s, (kvs, qkvm) in enumerate(((kvs0, qkvm0), (kvs1, qkvm1))):
        own_q = (q0, q1)[s]
        qs = all_four(x_xor, own_q)
        parts = token_attention(doc_ids, s, qs, kvs[2], kvs[1], kvs[-1], kvs[0])
        parts = [parts[0]] + [x_xor(parts[d], d) for d in (1, 2, 3)]
        attn = token_combine(own_q, qkvm, parts)
        blocks = gather_heads_relay(attn)
        if s == 0:
            hidden = token_out(blocks, cols, s, w_out)
        else:
            early = token_out_early(blocks[:4], cols, s, w_out)
            hidden = token_out_late(blocks[4], early, s, w_out, hidden)
    return hidden.transpose(0, 2, 1), finish(own, other)


def solution(mesh):
    return jax.shard_map(
        per_device,
        mesh=mesh,
        in_specs=(
            P(None, "seq", None),
            P(),
            P(),
            P(),
            P(None, "head"),
            P(None, "head"),
            P(None, "head"),
            P(None, "head"),
            P("head", None),
        ),
        out_specs=(P(None, "seq", "head"), P()),
        check_vma=False,
    )
```

```python
import functools
import math

import jax
import jax.numpy as jnp
from jax import lax
from jax.experimental import pallas as pl
from jax.experimental.pallas import tpu as pltpu
from jax.sharding import PartitionSpec as P


D = 3584
HD = 256
M = 32
ROWS = 256
COLS = 448
HALF = D // 2
KC = 512
SHAPE = 4
LOG2E_SCALE = math.log2(math.e) / 16.0
LOW = -1e30
BF = jnp.bfloat16
F32 = jnp.float32


WHOLE = pl.BlockSpec(memory_space=pltpu.VMEM)


def params(mib, **kw):
    return pltpu.CompilerParams(vmem_limit_bytes=mib * 1024 * 1024, **kw)


def dot(a, b):
    return jnp.dot(a, b, preferred_element_type=F32)


def dot_t(a, b):
    return lax.dot_general(a, b, (((1,), (1,)), ((), ())), preferred_element_type=F32)


def normed(rows, gain):
    v = rows.astype(F32)
    r = lax.rsqrt(jnp.mean(v * v, axis=-1, keepdims=True) + 1e-6)
    return (v * r * gain.astype(F32)).astype(BF)


def column(row):
    return jnp.broadcast_to(row, (128, row.shape[1])).T[:, :1]


def as_row(col):
    return jnp.broadcast_to(col, (col.shape[0], 128)).T[:1, :]


def attend(score_list, value_list):
    peak = functools.reduce(jnp.maximum, [jnp.max(s, axis=1, keepdims=True) for s in score_list])
    peak = jnp.maximum(peak, -1e29)
    total = 0.0
    mixed = 0.0
    for s, v in zip(score_list, value_list):
        p = jnp.exp2(s - peak)
        total = total + jnp.sum(p, axis=1, keepdims=True)
        mixed = mixed + dot(p.astype(BF), v)
    some = total > 0.0
    out = mixed / jnp.where(some, total, 1.0)
    return out, jnp.where(some, peak + jnp.log2(jnp.where(some, total, 1.0)), LOW)


def memory_part(qkvm, key_blocks, first, out_ref):
    for g in range(2):
        q = qkvm[:, g * HD : (g + 1) * HD]
        scores = [dot_t(q, kv[:, :HD]) * LOG2E_SCALE for kv in key_blocks]
        sm = dot_t(q, qkvm[:, 2 * HD : 3 * HD]) * LOG2E_SCALE
        scores.append(jnp.where(first, sm, LOW))
        out, lse = attend(scores, [kv[:, HD:] for kv in key_blocks] + [qkvm[:, 3 * HD :]])
        hi = lse.astype(BF)
        lo = (lse - hi.astype(F32)).astype(BF)
        lane = lax.broadcasted_iota(jnp.int32, (M, 128), 1)
        stats = jnp.where(lane == 0, hi.astype(F32), jnp.where(lane == 1, lo.astype(F32), 0.0))
        out_ref[g * M : (g + 1) * M, :HD] = out.astype(BF)
        out_ref[g * M : (g + 1) * M, HD:] = stats.astype(BF)


def place():
    i = lax.axis_index("seq")
    h = lax.axis_index("head")
    return i % SHAPE, i // SHAPE, h // 2, h % 2


def scaled_chunk(x, gain, squares, rows, first):
    v = x.astype(F32)
    sq = v * v
    part = sq[:, :128]
    for n in range(1, KC // 128):
        part = part + sq[:, n * 128 : (n + 1) * 128]
    squares[rows, :] = part if first else squares[rows, :] + part
    return (v * gain).astype(BF)


def norm_of(squares):
    return lax.rsqrt(jnp.sum(squares[...], axis=1, keepdims=True) / D + 1e-6)


def accumulate(acc, a, ws, first):
    at = 0
    for w in ws:
        span = slice(at, at + w.shape[1])
        part = dot(a, w)
        acc[:, span] = part if first else acc[:, span] + part
        at = at + w.shape[1]


def first_kernel(x, mem, gain, wq, wk, wv, q_ref, kv_ref, qkvm_ref, part_ref, *refs):
    bufs, (xs, ms, squares, acc, sems) = refs[:3], refs[3:]
    groups = []
    for k in range(D // KC):
        span = pl.ds(k * KC, KC)
        pairs = [(x.at[0, :, span], xs.at[:, span]), (mem.at[:, span], ms.at[:, span])]
        pairs += [(w.at[span, :], buf.at[span, :]) for w, buf in zip((wq, wk, wv), bufs)]
        groups.append(
            [pltpu.make_async_copy(p, q, sems.at[k, n]) for n, (p, q) in enumerate(pairs)]
        )
    for group in groups:
        for c in group:
            c.start()
    g = gain[...].astype(F32).reshape(1, D)
    for k, group in enumerate(groups):
        for c in group:
            c.wait()
        span = slice(k * KC, (k + 1) * KC)
        top = scaled_chunk(xs[:, span], g[:, span], squares, slice(0, ROWS), k == 0)
        low = scaled_chunk(ms[:, span], g[:, span], squares, slice(ROWS, ROWS + M), k == 0)
        a = jnp.concatenate([top, low], axis=0)
        accumulate(acc, a, [buf[span, :] for buf in bufs], k == 0)
    out = (acc[...] * norm_of(squares)).astype(BF)
    q_ref[...] = out[:ROWS, : 2 * HD]
    kv_ref[...] = out[:ROWS, 2 * HD :]
    qkvm_ref[...] = out[ROWS:, :]
    px, py, _, _ = place()
    memory_part(qkvm_ref[...], [kv_ref[...]], px + py == 0, part_ref)


def first_project(x, mem, gain, wq, wk, wv):
    hbm = pl.BlockSpec(memory_space=pltpu.HBM)
    shapes = [(ROWS, 2 * HD), (ROWS, 2 * HD), (M, 4 * HD), (2 * M, HD + 128)]
    shapes += [wq.shape, wk.shape, wv.shape]
    return pl.pallas_call(
        first_kernel,
        in_specs=[hbm, hbm, WHOLE, hbm, hbm, hbm],
        out_specs=[WHOLE] * len(shapes),
        out_shape=[jax.ShapeDtypeStruct(s, BF) for s in shapes],
        scratch_shapes=[
            pltpu.VMEM((ROWS, D), BF),
            pltpu.VMEM((M, D), BF),
            pltpu.VMEM((ROWS + M, 128), F32),
            pltpu.VMEM((ROWS + M, 4 * HD), F32),
            pltpu.SemaphoreType.DMA((D // KC, 5)),
        ],
        compiler_params=params(28),
        cost_estimate=pl.CostEstimate(
            flops=2 * (ROWS + M) * D * 4 * HD, bytes_accessed=10 * 2**20, transcendentals=512
        ),
        name="first_project",
    )(x, mem, gain, wq, wk, wv)


def window(h):
    return pl.multiple_of((h * 7 // 2) * 128, 128)


def second_kernel(x, gain, wq, wk, wv, wt, proj, *refs):
    q_ref, kv_ref, wt_buf, proj_buf, cols_buf, xs, squares, acc, sems, wsems = refs
    _, _, z, c = place()
    copies = []
    for k in range(D // KC):
        span = pl.ds(k * KC, KC)
        copies.append(pltpu.make_async_copy(x.at[1, :, span], xs.at[:, span], sems.at[k]))
    late = [
        pltpu.make_async_copy(src, dst, wsems.at[n])
        for n, (src, dst) in enumerate(
            (
                (wt, wt_buf),
                (proj, proj_buf),
                (x.at[:, :, pl.ds(window(2 * z + c), 512)], cols_buf),
            )
        )
    ]
    for c in copies + late:
        c.start()
    g = gain[...].astype(F32).reshape(1, D)
    for k, c in enumerate(copies):
        c.wait()
        span = slice(k * KC, (k + 1) * KC)
        a = scaled_chunk(xs[:, span], g[:, span], squares, slice(0, ROWS), k == 0)
        accumulate(acc, a, [w[span, :] for w in (wq, wk, wv)], k == 0)
    out = (acc[...] * norm_of(squares)).astype(BF)
    q_ref[...] = out[:, : 2 * HD]
    kv_ref[...] = out[:, 2 * HD :]
    for c in late:
        c.wait()


def second_project(x, gain, wq, wk, wv, wt, proj):
    hbm = pl.BlockSpec(memory_space=pltpu.HBM)
    shapes = [(ROWS, 2 * HD), (ROWS, 2 * HD), wt.shape, proj.shape, (2, ROWS, 512)]
    return pl.pallas_call(
        second_kernel,
        in_specs=[hbm] + [WHOLE] * 4 + [hbm, hbm],
        out_specs=[WHOLE] * len(shapes),
        out_shape=[jax.ShapeDtypeStruct(s, BF) for s in shapes],
        scratch_shapes=[
            pltpu.VMEM((ROWS, D), BF),
            pltpu.VMEM((ROWS, 128), F32),
            pltpu.VMEM((ROWS, 4 * HD), F32),
            pltpu.SemaphoreType.DMA((D // KC,)),
            pltpu.SemaphoreType.DMA((3,)),
        ],
        compiler_params=params(28),
        cost_estimate=pl.CostEstimate(
            flops=2 * ROWS * D * 4 * HD, bytes_accessed=10 * 2**20, transcendentals=512
        ),
        name="second_project",
    )(x, gain, wq, wk, wv, wt, proj)


def memory_project_kernel(own, other, gain, wq, wk, wv, *refs):
    kvs, (qkvm_ref, part_ref, whole_ref) = refs[:4], refs[4:]
    px, _, _, c = place()
    whole_ref[:, pl.ds(pl.multiple_of(c * HALF, 128), HALF)] = own[...]
    whole_ref[:, pl.ds(pl.multiple_of((1 - c) * HALF, 128), HALF)] = other[...]
    a = normed(whole_ref[...], gain[...].reshape(1, D))
    qkvm_ref[:, : 2 * HD] = dot(a, wq[...]).astype(BF)
    qkvm_ref[:, 2 * HD : 3 * HD] = dot(a, wk[...]).astype(BF)
    qkvm_ref[:, 3 * HD :] = dot(a, wv[...]).astype(BF)
    memory_part(qkvm_ref[...], [kv[...] for kv in kvs], px == 0, part_ref)


def memory_project(own, other, gain, wq, wk, wv, kvs):
    return pl.pallas_call(
        memory_project_kernel,
        in_specs=[WHOLE] * 10,
        out_specs=[WHOLE] * 3,
        out_shape=[
            jax.ShapeDtypeStruct((M, 4 * HD), BF),
            jax.ShapeDtypeStruct((2 * M, HD + 128), BF),
            jax.ShapeDtypeStruct((M, D), BF),
        ],
        compiler_params=params(20),
        cost_estimate=pl.CostEstimate(
            flops=2 * 256 * D * 4 * HD, bytes_accessed=8 * 1024 * 1024, transcendentals=M
        ),
        name="memory_project",
    )(own, other, gain, wq, wk, wv, *kvs)


def memory_combine_kernel(last, a, b, out_ref):
    parts = [r[...].astype(F32) for r in (a, b)]
    lses = [p[:, HD : HD + 1] + p[:, HD + 1 : HD + 2] for p in parts]
    peak = functools.reduce(jnp.maximum, lses)
    ws = [jnp.exp2(s - peak) for s in lses]
    total = sum(ws)
    out = sum(w * p[:, :HD] for w, p in zip(ws, parts)) / total
    if last:
        out_ref[:, :HD] = out[:M].astype(BF)
        out_ref[:, HD:] = out[M:].astype(BF)
    else:
        lse = peak + jnp.log2(total)
        hi = lse.astype(BF).astype(F32)
        lane = lax.broadcasted_iota(jnp.int32, (2 * M, 128), 1)
        stats = jnp.where(lane == 0, hi, jnp.where(lane == 1, lse - hi, 0.0))
        out_ref[:, :HD] = out.astype(BF)
        out_ref[:, HD:] = stats.astype(BF)


def memory_combine(a, b, last=False):
    shape = (M, 2 * HD) if last else (2 * M, HD + 128)
    return pl.pallas_call(
        functools.partial(memory_combine_kernel, last),
        in_specs=[WHOLE] * 2,
        out_specs=WHOLE,
        out_shape=jax.ShapeDtypeStruct(shape, BF),
        compiler_params=params(4),
        cost_estimate=pl.CostEstimate(flops=10**8, bytes_accessed=10**5, transcendentals=256),
        name="memory_combine",
    )(a, b)


def pair_kernel(a, b, out_ref):
    out_ref[0] = a[...]
    out_ref[1] = b[...]


def pair_up(a, b):
    return pl.pallas_call(
        pair_kernel,
        in_specs=[WHOLE] * 2,
        out_specs=WHOLE,
        out_shape=jax.ShapeDtypeStruct((2, *a.shape), BF),
        compiler_params=params(4),
        name="pair_up",
    )(a, b)


def first_kernel_of(v, out_ref):
    out_ref[...] = v[0]


def first_of(v):
    return pl.pallas_call(
        first_kernel_of,
        in_specs=[WHOLE],
        out_specs=WHOLE,
        out_shape=jax.ShapeDtypeStruct(v.shape[1:], BF),
        compiler_params=params(4),
        name="first_of",
    )(v)


def gathered_heads():
    _, _, z, c = place()
    side = 1 - 2 * c
    before, after = lax.rem(z - side + SHAPE, SHAPE), lax.rem(z + side + SHAPE, SHAPE)
    far = lax.rem(z + 2, SHAPE)
    chips = (z, z, before, before, after, after, far, far)
    cores = (c, 1 - c, c, 1 - c, 1 - c, c, c, 1 - c)
    return [2 * zz + cc for zz, cc in zip(chips, cores)]


def block_values(refs):
    own, swapped, near, near2, far, far2 = refs
    return [own[...], swapped[...], near[0], near[1], near2[0], near2[1], far[...], far2[...]]


def memory_write_kernel(o, o2, n, n2, f, f2, mem, w_out, proj, keep_ref, send_ref):
    _, _, z, c = place()
    wide = mem[:, pl.ds(window(2 * z + c), 512)].astype(F32)
    acc = jnp.where(c == 1, wide[:, 64:], wide[:, :COLS])
    for h, v in zip(gathered_heads(), block_values((o, o2, n, n2, f, f2))):
        acc = acc + dot_t(v, w_out[:, pl.ds(pl.multiple_of(h * 2 * HD, 2 * HD), 2 * HD)])
    a = acc.astype(BF)
    keep_ref[...] = dot(a, proj[:, pl.ds(pl.multiple_of(c * HALF, 128), HALF)]).astype(BF)
    send_ref[...] = dot(a, proj[:, pl.ds(pl.multiple_of((1 - c) * HALF, 128), HALF)]).astype(BF)


def finish_kernel(own, other, out_ref):
    _, _, _, c = place()
    out_ref[:, pl.ds(pl.multiple_of(c * HALF, 128), HALF)] = own[...]
    out_ref[:, pl.ds(pl.multiple_of((1 - c) * HALF, 128), HALF)] = other[...]


def finish(own, other):
    return pl.pallas_call(
        finish_kernel,
        in_specs=[WHOLE] * 2,
        out_specs=WHOLE,
        out_shape=jax.ShapeDtypeStruct((M, D), BF),
        compiler_params=params(4),
        name="finish",
    )(own, other)


def memory_write(blocks, mem, w_out, proj):
    return pl.pallas_call(
        memory_write_kernel,
        in_specs=[WHOLE] * 9,
        out_specs=[WHOLE] * 2,
        out_shape=[jax.ShapeDtypeStruct((M, HALF), BF)] * 2,
        compiler_params=params(20),
        cost_estimate=pl.CostEstimate(
            flops=2 * 256 * D * 8 * COLS, bytes_accessed=8 * 1024 * 1024, transcendentals=0
        ),
        name="memory_write",
    )(*blocks, mem, w_out, proj)


def stack_kernel(kva, kvb, kvb2, kvc, kvs, send):
    x, y, _, _ = place()
    kvs[:ROWS, :] = kva[...]
    kvs[ROWS : 2 * ROWS, :] = jnp.where(y % 2 == 1, kvb[...], kvb2[...])
    kvs[2 * ROWS :, :] = kvc[...]
    at = pl.multiple_of(jnp.where(x >= 2, 0, ROWS), ROWS)
    send[...] = kvs[pl.ds(at, 2 * ROWS), :]


def stack(kva, kvb, kvb2, kvc):
    return pl.pallas_call(
        stack_kernel,
        in_specs=[WHOLE] * 4,
        out_specs=[WHOLE] * 2,
        out_shape=[
            jax.ShapeDtypeStruct((3 * ROWS, 2 * HD), BF),
            jax.ShapeDtypeStruct((2 * ROWS, 2 * HD), BF),
        ],
        compiler_params=params(8),
        name="stack",
    )(kva, kvb, kvb2, kvc)


def token_kernel(seg, docs, q0, q1, kvs, far_kvs, o0, o1, kcode):
    x, y, _, _ = place()
    lane = lax.broadcasted_iota(jnp.int32, (1, ROWS), 1).astype(F32)

    def codes_of(block):
        start = jnp.maximum(block, 0) * ROWS
        doc = docs[seg : seg + 1, pl.ds(pl.multiple_of(start, ROWS), ROWS)].astype(F32)
        return doc * 4096.0, doc * 4096.0 + lane + start.astype(F32)

    first_row = jnp.where(x >= 2, y - 1, y - 2)
    blocks = [(y - 2 + n) * SHAPE + x for n in range(3)]
    blocks += [(first_row + n) * SHAPE + (SHAPE - 1 - x) for n in range(2)]
    for n, block in enumerate(blocks):
        code = codes_of(block)[1]
        kcode[:, n * ROWS : (n + 1) * ROWS] = jnp.where(block >= 0, code, -1.0)
    near = lax.bitwise_xor(x, 1)
    for e, (q_ref, o_ref) in enumerate(((q0, o0), (q1, o1))):
        low, high = codes_of(y * SHAPE + (x if e == 0 else near))
        low, high = column(low), column(high)
        if e == 0:
            span = slice(0, 3 * ROWS)
        else:
            span = pl.ds(pl.multiple_of(jnp.where(near < x, 0, ROWS), ROWS), 2 * ROWS)
        keys = [kvs[span, :], far_kvs[...]]
        codes = [kcode[:, span], kcode[:, 3 * ROWS :]]
        valid = [(k >= low) & (k <= high) for k in codes]
        for g in range(2):
            q = q_ref[:, g * HD : (g + 1) * HD]
            scores = [
                jnp.where(v, dot_t(q, k[:, :HD]) * LOG2E_SCALE, LOW) for v, k in zip(valid, keys)
            ]
            out, lse = attend(scores, [k[:, HD:] for k in keys])
            row = as_row(lse)
            hi = row.astype(BF).astype(F32)
            sub = lax.broadcasted_iota(jnp.int32, (16, ROWS), 0)
            stats = jnp.where(sub == 0, hi, jnp.where(sub == 1, row - hi, 0.0))
            o_ref[:ROWS, g * HD : (g + 1) * HD] = out.astype(BF)
            o_ref[ROWS:, g * HD : (g + 1) * HD] = stats.astype(BF)


def token_attention(docs, seg, q, near_q, kvs, far_kvs):
    return pl.pallas_call(
        functools.partial(token_kernel, seg),
        in_specs=[WHOLE] * 5,
        out_specs=[WHOLE] * 2,
        out_shape=[jax.ShapeDtypeStruct((ROWS + 16, 2 * HD), BF)] * 2,
        scratch_shapes=[pltpu.VMEM((1, 5 * ROWS), F32)],
        compiler_params=params(16),
        cost_estimate=pl.CostEstimate(
            flops=3 * 10**9, bytes_accessed=4 * 10**6, transcendentals=10**6
        ),
        name="token_attention",
    )(docs, q, near_q, kvs, far_kvs)


def token_combine_kernel(q, qkvm, a, b, out_ref):
    refs = (a, b)
    for g in range(2):
        lanes = slice(g * HD, (g + 1) * HD)
        scores = dot_t(q[:, lanes], qkvm[:, 2 * HD : 3 * HD]) * LOG2E_SCALE
        out, lse = attend([scores], [qkvm[:, 3 * HD :]])
        outs, lses = [out], [lse]
        for r in refs:
            tail = r[ROWS:, lanes].astype(F32)
            lses.append(column(tail[0:1, :] + tail[1:2, :]))
            outs.append(r[:ROWS, lanes].astype(F32))
        peak = functools.reduce(jnp.maximum, lses)
        ws = [jnp.exp2(s - peak) for s in lses]
        mixed = sum(w * o for w, o in zip(ws, outs)) / sum(ws)
        out_ref[:, lanes] = mixed.astype(BF)


def token_combine(q, qkvm, parts):
    return pl.pallas_call(
        token_combine_kernel,
        in_specs=[WHOLE] * 4,
        out_specs=WHOLE,
        out_shape=jax.ShapeDtypeStruct((ROWS, 2 * HD), BF),
        compiler_params=params(12),
        cost_estimate=pl.CostEstimate(flops=5 * 10**8, bytes_accessed=10**6, transcendentals=4096),
        name="token_combine",
    )(q, qkvm, *parts)


def token_out_kernel(seg, *refs):
    blocks, cols, w_out, out_ref, flat = refs[:6], *refs[6:]
    acc = features(cols, seg, flat)
    for h, v in zip(gathered_heads(), block_values(blocks)):
        acc = acc + dot_t(w_out[:, pl.ds(pl.multiple_of(h * 2 * HD, 2 * HD), 2 * HD)], v)
    out_ref[0] = acc.astype(BF)


def features(cols, seg, flat):
    _, _, _, c = place()
    for at in range(0, 512, 128):
        flat[at : at + 128, :] = cols[seg, :, at : at + 128].astype(F32).T
    return flat[pl.ds(pl.multiple_of(c * 64, 64), COLS), :]


def token_out(blocks, cols, seg, w_out):
    return pl.pallas_call(
        functools.partial(token_out_kernel, seg),
        grid=(1,),
        in_specs=[WHOLE] * 8,
        out_specs=pl.BlockSpec((1, COLS, ROWS), lambda k: (seg, 0, 0)),
        out_shape=jax.ShapeDtypeStruct((2, COLS, ROWS), BF),
        scratch_shapes=[pltpu.VMEM((512, ROWS), F32)],
        compiler_params=params(12),
        cost_estimate=pl.CostEstimate(
            flops=2 * ROWS * 4096 * COLS, bytes_accessed=6 * 10**6, transcendentals=0
        ),
        name="token_out",
    )(*blocks, cols, w_out)


def early_kernel(seg, *refs):
    cols, w_out, out_ref, flat = refs[4:]
    own, swapped, near, near2 = refs[:4]
    values = [own[...], swapped[...], near[0], near[1], near2[0], near2[1]]
    acc = features(cols, seg, flat)
    for h, v in zip(gathered_heads(), values):
        acc = acc + dot_t(w_out[:, pl.ds(pl.multiple_of(h * 2 * HD, 2 * HD), 2 * HD)], v)
    out_ref[...] = acc


def token_out_early(blocks, cols, seg, w_out):
    return pl.pallas_call(
        functools.partial(early_kernel, seg),
        in_specs=[WHOLE] * 6,
        out_specs=WHOLE,
        out_shape=jax.ShapeDtypeStruct((COLS, ROWS), F32),
        scratch_shapes=[pltpu.VMEM((512, ROWS), F32)],
        compiler_params=params(12),
        cost_estimate=pl.CostEstimate(
            flops=2 * ROWS * 3072 * COLS, bytes_accessed=5 * 10**6, transcendentals=0
        ),
        name="token_out_early",
    )(*blocks, cols, w_out)


def late_kernel(far, far2, early, w_out, before, out_ref):
    acc = early[...]
    for h, v in zip(gathered_heads()[6:], (far[...], far2[...])):
        acc = acc + dot_t(w_out[:, pl.ds(pl.multiple_of(h * 2 * HD, 2 * HD), 2 * HD)], v)
    out_ref[0] = acc.astype(BF)


def token_out_late(far, far2, early, seg, w_out, before):
    return pl.pallas_call(
        late_kernel,
        grid=(1,),
        in_specs=[WHOLE] * 4 + [pl.BlockSpec(memory_space=pl.ANY)],
        out_specs=pl.BlockSpec((1, COLS, ROWS), lambda k: (seg, 0, 0)),
        out_shape=jax.ShapeDtypeStruct((2, COLS, ROWS), BF),
        input_output_aliases={4: 0},
        compiler_params=params(12),
        cost_estimate=pl.CostEstimate(
            flops=2 * ROWS * 1024 * COLS, bytes_accessed=3 * 10**6, transcendentals=0
        ),
        name="token_out_late",
    )(far, far2, early, w_out, before)


N_SEQ, N_HEAD = SHAPE * SHAPE, 8


def x_xor(v, d):
    return lax.ppermute(v, "seq", [(i, i ^ d) for i in range(N_SEQ)])


def y_xor(v, d):
    return x_xor(v, 4 * d)


def y_later(v):
    return lax.ppermute(v, "seq", [(i, i + SHAPE) for i in range(N_SEQ - SHAPE)])


def all_four(send, v):
    near = send(v, 1)
    return [v, near, send(near, 3), send(v, 3)]


def x_near(v):
    return lax.ppermute(v, "seq", [(i, i ^ 1) for i in range(N_SEQ)])


def x_far(v):
    return lax.ppermute(v, "seq", [(i, i ^ 3) for i in range(N_SEQ)])


def y_near(v):
    return lax.ppermute(v, "seq", [(i, i ^ 4) for i in range(N_SEQ)])


def y_far(v):
    return lax.ppermute(v, "seq", [(i, i ^ 12) for i in range(N_SEQ)])


def z_xor(v, d):
    return lax.ppermute(v, "head", [(i, i ^ (2 * d)) for i in range(N_HEAD)])


def z_turn(v):
    return lax.ppermute(v, "head", [(i, (i + 2 - 4 * (i % 2)) % N_HEAD) for i in range(N_HEAD)])


def other_core(v):
    return lax.ppermute(v, "head", [(i, i ^ 1) for i in range(N_HEAD)])


def add(a, b):
    return (a.astype(F32) + b.astype(F32)).astype(BF)


def gather_heads_direct(v):
    far = z_xor(v, 2)
    swapped = other_core(v)
    near = z_turn(pair_up(v, swapped))
    near2 = other_core(near)
    return v, swapped, near, near2, far, other_core(far)


def gather_heads(v):
    swapped = other_core(v)
    near = z_turn(pair_up(v, swapped))
    far = z_turn(first_of(near))
    near2 = other_core(near)
    return v, swapped, near, near2, far, other_core(far)


def memory_tail(attn, mem, w_out, proj):
    blocks = gather_heads_direct(attn)
    keep, send = memory_write(blocks, mem, w_out, proj)
    half = add(keep, other_core(send))
    near, far, two = [z_xor(half, d) for d in (1, 3, 2)]
    half = ((half.astype(F32) + near.astype(F32)) + (far.astype(F32) + two.astype(F32))).astype(BF)
    return half, other_core(half)


def per_device(segment_input, doc_ids, memory, gain, w_query, w_key, w_value, w_out, mem_proj):
    in_hbm = lambda v: pltpu.with_memory_space_constraint(v, pltpu.HBM)
    x = in_hbm(segment_input)

    q0, kv0, qkvm0, part, *weights = first_project(
        x, in_hbm(memory), gain, *[in_hbm(w) for w in (w_query, w_key, w_value)]
    )
    weights = (gain, *weights)
    q1, kv1, w_out, mem_proj, cols = second_project(x, *weights, in_hbm(w_out.T), in_hbm(mem_proj))

    part = memory_combine(part, x_near(part))
    part = memory_combine(part, x_far(part))
    part = memory_combine(part, y_near(part))
    attn = memory_combine(part, y_far(part), True)
    own, other = memory_tail(attn, memory, w_out, mem_proj)

    next_row = y_later(kv0)
    kvs0 = [kv0, next_row, y_later(next_row), next_row]
    kvs1 = all_four(y_xor, kv1)
    qkvm1, part, mem1 = memory_project(own, other, *weights, kvs1)
    part = memory_combine(part, x_near(part))
    attn = memory_combine(part, x_far(part), True)
    own, other = memory_tail(attn, mem1, w_out, mem_proj)

    for s, (kvs, qkvm) in enumerate(((kvs0, qkvm0), (kvs1, qkvm1))):
        own_q = (q0, q1)[s]
        near_q = x_xor(own_q, 1)
        stacked, send = stack(kvs[2], kvs[1], kvs[-1], kvs[0])
        far_kvs = x_xor(send, 3)
        mine, send = token_attention(doc_ids, s, own_q, near_q, stacked, far_kvs)
        parts = [mine, x_xor(send, 1)]
        attn = token_combine(own_q, qkvm, parts)
        blocks = gather_heads(attn)
        if s == 0:
            hidden = token_out(blocks, cols, s, w_out)
        else:
            early = token_out_early(blocks[:4], cols, s, w_out)
            hidden = token_out_late(*blocks[4:], early, s, w_out, hidden)
    return hidden.transpose(0, 2, 1), finish(own, other)


def solution(mesh):
    return jax.shard_map(
        per_device,
        mesh=mesh,
        in_specs=(
            P(None, "seq", None),
            P(),
            P(),
            P(),
            P(None, "head"),
            P(None, "head"),
            P(None, "head"),
            P(None, "head"),
            P("head", None),
        ),
        out_specs=(P(None, "seq", "head"), P()),
        check_vma=False,
    )
```

```python
import functools
import math

import jax
import jax.numpy as jnp
from jax import lax
from jax.experimental import pallas as pl
from jax.experimental.pallas import tpu as pltpu
from jax.sharding import PartitionSpec as P


D = 3584
HD = 256
M = 32
ROWS = 256
COLS = 448
HALF = D // 2
KC = 512
SHAPE = 4
LOG2E_SCALE = math.log2(math.e) / 16.0
LOW = -1e30
BF = jnp.bfloat16
F32 = jnp.float32


WHOLE = pl.BlockSpec(memory_space=pltpu.VMEM)


def params(mib, **kw):
    return pltpu.CompilerParams(vmem_limit_bytes=mib * 1024 * 1024, **kw)


def dot(a, b):
    return jnp.dot(a, b, preferred_element_type=F32)


def dot_t(a, b):
    return lax.dot_general(a, b, (((1,), (1,)), ((), ())), preferred_element_type=F32)


def normed(rows, gain):
    v = rows.astype(F32)
    r = lax.rsqrt(jnp.mean(v * v, axis=-1, keepdims=True) + 1e-6)
    return (v * r * gain.astype(F32)).astype(BF)


def column(row):
    return jnp.broadcast_to(row, (128, row.shape[1])).T[:, :1]


def as_row(col):
    return jnp.broadcast_to(col, (col.shape[0], 128)).T[:1, :]


def attend(score_list, value_list):
    peak = functools.reduce(jnp.maximum, [jnp.max(s, axis=1, keepdims=True) for s in score_list])
    peak = jnp.maximum(peak, -1e29)
    total = 0.0
    mixed = 0.0
    for s, v in zip(score_list, value_list):
        p = jnp.exp2(s - peak)
        total = total + jnp.sum(p, axis=1, keepdims=True)
        mixed = mixed + dot(p.astype(BF), v)
    some = total > 0.0
    out = mixed / jnp.where(some, total, 1.0)
    return out, jnp.where(some, peak + jnp.log2(jnp.where(some, total, 1.0)), LOW)


def memory_part(qkvm, key_blocks, first, out_ref):
    for g in range(2):
        q = qkvm[:, g * HD : (g + 1) * HD]
        scores = [dot_t(q, kv[:, :HD]) * LOG2E_SCALE for kv in key_blocks]
        sm = dot_t(q, qkvm[:, 2 * HD : 3 * HD]) * LOG2E_SCALE
        scores.append(jnp.where(first, sm, LOW))
        out, lse = attend(scores, [kv[:, HD:] for kv in key_blocks] + [qkvm[:, 3 * HD :]])
        hi = lse.astype(BF)
        lo = (lse - hi.astype(F32)).astype(BF)
        lane = lax.broadcasted_iota(jnp.int32, (M, 128), 1)
        stats = jnp.where(lane == 0, hi.astype(F32), jnp.where(lane == 1, lo.astype(F32), 0.0))
        out_ref[g * M : (g + 1) * M, :HD] = out.astype(BF)
        out_ref[g * M : (g + 1) * M, HD:] = stats.astype(BF)


def place():
    i = lax.axis_index("seq")
    h = lax.axis_index("head")
    return i % SHAPE, i // SHAPE, h // 2, h % 2


def scaled_chunk(x, gain, squares, rows, first):
    v = x.astype(F32)
    sq = v * v
    part = sq[:, :128]
    for n in range(1, KC // 128):
        part = part + sq[:, n * 128 : (n + 1) * 128]
    squares[rows, :] = part if first else squares[rows, :] + part
    return (v * gain).astype(BF)


def norm_of(squares):
    return lax.rsqrt(jnp.sum(squares[...], axis=1, keepdims=True) / D + 1e-6)


def accumulate(acc, a, ws, first):
    at = 0
    for w in ws:
        span = slice(at, at + w.shape[1])
        part = dot(a, w)
        acc[:, span] = part if first else acc[:, span] + part
        at = at + w.shape[1]


def first_kernel(x, mem, gain, wq, wk, wv, q_ref, kv_ref, qkvm_ref, part_ref, *refs):
    bufs, (xs, ms, squares, acc, sems) = refs[:3], refs[3:]
    groups = []
    for k in range(D // KC):
        span = pl.ds(k * KC, KC)
        pairs = [(x.at[0, :, span], xs.at[:, span]), (mem.at[:, span], ms.at[:, span])]
        pairs += [(w.at[span, :], buf.at[span, :]) for w, buf in zip((wq, wk, wv), bufs)]
        groups.append(
            [pltpu.make_async_copy(p, q, sems.at[k, n]) for n, (p, q) in enumerate(pairs)]
        )
    for group in groups:
        for c in group:
            c.start()
    g = gain[...].astype(F32).reshape(1, D)
    for k, group in enumerate(groups):
        for c in group:
            c.wait()
        span = slice(k * KC, (k + 1) * KC)
        top = scaled_chunk(xs[:, span], g[:, span], squares, slice(0, ROWS), k == 0)
        low = scaled_chunk(ms[:, span], g[:, span], squares, slice(ROWS, ROWS + M), k == 0)
        a = jnp.concatenate([top, low], axis=0)
        accumulate(acc, a, [buf[span, :] for buf in bufs], k == 0)
    out = (acc[...] * norm_of(squares)).astype(BF)
    q_ref[...] = out[:ROWS, : 2 * HD]
    kv_ref[...] = out[:ROWS, 2 * HD :]
    qkvm_ref[...] = out[ROWS:, :]
    px, py, _, _ = place()
    memory_part(qkvm_ref[...], [kv_ref[...]], px + py == 0, part_ref)


def first_project(x, mem, gain, wq, wk, wv):
    hbm = pl.BlockSpec(memory_space=pltpu.HBM)
    shapes = [(ROWS, 2 * HD), (ROWS, 2 * HD), (M, 4 * HD), (2 * M, HD + 128)]
    shapes += [wq.shape, wk.shape, wv.shape]
    return pl.pallas_call(
        first_kernel,
        in_specs=[hbm, hbm, WHOLE, hbm, hbm, hbm],
        out_specs=[WHOLE] * len(shapes),
        out_shape=[jax.ShapeDtypeStruct(s, BF) for s in shapes],
        scratch_shapes=[
            pltpu.VMEM((ROWS, D), BF),
            pltpu.VMEM((M, D), BF),
            pltpu.VMEM((ROWS + M, 128), F32),
            pltpu.VMEM((ROWS + M, 4 * HD), F32),
            pltpu.SemaphoreType.DMA((D // KC, 5)),
        ],
        compiler_params=params(28),
        cost_estimate=pl.CostEstimate(
            flops=2 * (ROWS + M) * D * 4 * HD, bytes_accessed=10 * 2**20, transcendentals=512
        ),
        name="first_project",
    )(x, mem, gain, wq, wk, wv)


def window(h):
    return pl.multiple_of((h * 7 // 2) * 128, 128)


def second_kernel(x, gain, wq, wk, wv, wt, proj, *refs):
    q_ref, kv_ref, wt_buf, proj_buf, cols_buf, xs, squares, acc, sems, wsems = refs
    _, _, z, c = place()
    copies = []
    for k in range(D // KC):
        span = pl.ds(k * KC, KC)
        copies.append(pltpu.make_async_copy(x.at[1, :, span], xs.at[:, span], sems.at[k]))
    late = [
        pltpu.make_async_copy(src, dst, wsems.at[n])
        for n, (src, dst) in enumerate(
            (
                (wt, wt_buf),
                (proj, proj_buf),
                (x.at[:, :, pl.ds(window(2 * z + c), 512)], cols_buf),
            )
        )
    ]
    for c in copies + late:
        c.start()
    g = gain[...].astype(F32).reshape(1, D)
    for k, c in enumerate(copies):
        c.wait()
        span = slice(k * KC, (k + 1) * KC)
        a = scaled_chunk(xs[:, span], g[:, span], squares, slice(0, ROWS), k == 0)
        accumulate(acc, a, [w[span, :] for w in (wq, wk, wv)], k == 0)
    out = (acc[...] * norm_of(squares)).astype(BF)
    q_ref[...] = out[:, : 2 * HD]
    kv_ref[...] = out[:, 2 * HD :]
    for c in late:
        c.wait()


def second_project(x, gain, wq, wk, wv, wt, proj):
    hbm = pl.BlockSpec(memory_space=pltpu.HBM)
    shapes = [(ROWS, 2 * HD), (ROWS, 2 * HD), wt.shape, proj.shape, (2, ROWS, 512)]
    return pl.pallas_call(
        second_kernel,
        in_specs=[hbm] + [WHOLE] * 4 + [hbm, hbm],
        out_specs=[WHOLE] * len(shapes),
        out_shape=[jax.ShapeDtypeStruct(s, BF) for s in shapes],
        scratch_shapes=[
            pltpu.VMEM((ROWS, D), BF),
            pltpu.VMEM((ROWS, 128), F32),
            pltpu.VMEM((ROWS, 4 * HD), F32),
            pltpu.SemaphoreType.DMA((D // KC,)),
            pltpu.SemaphoreType.DMA((3,)),
        ],
        compiler_params=params(28),
        cost_estimate=pl.CostEstimate(
            flops=2 * ROWS * D * 4 * HD, bytes_accessed=10 * 2**20, transcendentals=512
        ),
        name="second_project",
    )(x, gain, wq, wk, wv, wt, proj)


def memory_project_kernel(own, other, gain, wq, wk, wv, *refs):
    kvs, (qkvm_ref, part_ref, whole_ref) = refs[:4], refs[4:]
    px, _, _, c = place()
    whole_ref[:, pl.ds(pl.multiple_of(c * HALF, 128), HALF)] = own[...]
    whole_ref[:, pl.ds(pl.multiple_of((1 - c) * HALF, 128), HALF)] = other[...]
    a = normed(whole_ref[...], gain[...].reshape(1, D))
    qkvm_ref[:, : 2 * HD] = dot(a, wq[...]).astype(BF)
    qkvm_ref[:, 2 * HD : 3 * HD] = dot(a, wk[...]).astype(BF)
    qkvm_ref[:, 3 * HD :] = dot(a, wv[...]).astype(BF)
    memory_part(qkvm_ref[...], [kv[...] for kv in kvs], px == 0, part_ref)


def memory_project(own, other, gain, wq, wk, wv, kvs):
    return pl.pallas_call(
        memory_project_kernel,
        in_specs=[WHOLE] * 10,
        out_specs=[WHOLE] * 3,
        out_shape=[
            jax.ShapeDtypeStruct((M, 4 * HD), BF),
            jax.ShapeDtypeStruct((2 * M, HD + 128), BF),
            jax.ShapeDtypeStruct((M, D), BF),
        ],
        compiler_params=params(20),
        cost_estimate=pl.CostEstimate(
            flops=2 * 256 * D * 4 * HD, bytes_accessed=8 * 1024 * 1024, transcendentals=M
        ),
        name="memory_project",
    )(own, other, gain, wq, wk, wv, *kvs)


def memory_combine_kernel(last, a, b, out_ref):
    parts = [r[...].astype(F32) for r in (a, b)]
    lses = [p[:, HD : HD + 1] + p[:, HD + 1 : HD + 2] for p in parts]
    peak = functools.reduce(jnp.maximum, lses)
    ws = [jnp.exp2(s - peak) for s in lses]
    total = sum(ws)
    out = sum(w * p[:, :HD] for w, p in zip(ws, parts)) / total
    if last:
        out_ref[:, :HD] = out[:M].astype(BF)
        out_ref[:, HD:] = out[M:].astype(BF)
    else:
        lse = peak + jnp.log2(total)
        hi = lse.astype(BF).astype(F32)
        lane = lax.broadcasted_iota(jnp.int32, (2 * M, 128), 1)
        stats = jnp.where(lane == 0, hi, jnp.where(lane == 1, lse - hi, 0.0))
        out_ref[:, :HD] = out.astype(BF)
        out_ref[:, HD:] = stats.astype(BF)


def memory_combine(a, b, last=False):
    shape = (M, 2 * HD) if last else (2 * M, HD + 128)
    return pl.pallas_call(
        functools.partial(memory_combine_kernel, last),
        in_specs=[WHOLE] * 2,
        out_specs=WHOLE,
        out_shape=jax.ShapeDtypeStruct(shape, BF),
        compiler_params=params(4),
        cost_estimate=pl.CostEstimate(flops=10**8, bytes_accessed=10**5, transcendentals=256),
        name="memory_combine",
    )(a, b)


def pair_kernel(a, b, out_ref):
    out_ref[0] = a[...]
    out_ref[1] = b[...]


def pair_up(a, b):
    return pl.pallas_call(
        pair_kernel,
        in_specs=[WHOLE] * 2,
        out_specs=WHOLE,
        out_shape=jax.ShapeDtypeStruct((2, *a.shape), BF),
        compiler_params=params(4),
        name="pair_up",
    )(a, b)


def first_kernel_of(v, out_ref):
    out_ref[...] = v[0]


def first_of(v):
    return pl.pallas_call(
        first_kernel_of,
        in_specs=[WHOLE],
        out_specs=WHOLE,
        out_shape=jax.ShapeDtypeStruct(v.shape[1:], BF),
        compiler_params=params(4),
        name="first_of",
    )(v)


def gathered_heads():
    _, _, z, c = place()
    side = 1 - 2 * c
    before, after = lax.rem(z - side + SHAPE, SHAPE), lax.rem(z + side + SHAPE, SHAPE)
    far = lax.rem(z + 2, SHAPE)
    chips = (z, z, before, before, after, after, far, far)
    cores = (c, 1 - c, c, 1 - c, 1 - c, c, c, 1 - c)
    return [2 * zz + cc for zz, cc in zip(chips, cores)]


def block_values(refs):
    own, swapped, near, near2, far, far2 = refs
    return [own[...], swapped[...], near[0], near[1], near2[0], near2[1], far[...], far2[...]]


def memory_write_kernel(o, o2, n, n2, f, f2, mem, w_out, proj, keep_ref, send_ref):
    _, _, z, c = place()
    wide = mem[:, pl.ds(window(2 * z + c), 512)].astype(F32)
    acc = jnp.where(c == 1, wide[:, 64:], wide[:, :COLS])
    for h, v in zip(gathered_heads(), block_values((o, o2, n, n2, f, f2))):
        acc = acc + dot_t(v, w_out[:, pl.ds(pl.multiple_of(h * 2 * HD, 2 * HD), 2 * HD)])
    a = acc.astype(BF)
    keep_ref[...] = dot(a, proj[:, pl.ds(pl.multiple_of(c * HALF, 128), HALF)]).astype(BF)
    send_ref[...] = dot(a, proj[:, pl.ds(pl.multiple_of((1 - c) * HALF, 128), HALF)]).astype(BF)


def finish_kernel(own, other, out_ref):
    _, _, _, c = place()
    out_ref[:, pl.ds(pl.multiple_of(c * HALF, 128), HALF)] = own[...]
    out_ref[:, pl.ds(pl.multiple_of((1 - c) * HALF, 128), HALF)] = other[...]


def finish(own, other):
    return pl.pallas_call(
        finish_kernel,
        in_specs=[WHOLE] * 2,
        out_specs=WHOLE,
        out_shape=jax.ShapeDtypeStruct((M, D), BF),
        compiler_params=params(4),
        name="finish",
    )(own, other)


def memory_write(blocks, mem, w_out, proj):
    return pl.pallas_call(
        memory_write_kernel,
        in_specs=[WHOLE] * 9,
        out_specs=[WHOLE] * 2,
        out_shape=[jax.ShapeDtypeStruct((M, HALF), BF)] * 2,
        compiler_params=params(20),
        cost_estimate=pl.CostEstimate(
            flops=2 * 256 * D * 8 * COLS, bytes_accessed=8 * 1024 * 1024, transcendentals=0
        ),
        name="memory_write",
    )(*blocks, mem, w_out, proj)


def stack_kernel(kva, kvb, kvb2, kvc, kvs, send):
    x, y, _, _ = place()
    kvs[:ROWS, :] = kva[...]
    kvs[ROWS : 2 * ROWS, :] = jnp.where(y % 2 == 1, kvb[...], kvb2[...])
    kvs[2 * ROWS :, :] = kvc[...]
    at = pl.multiple_of(jnp.where(x >= 2, 0, ROWS), ROWS)
    send[...] = kvs[pl.ds(at, 2 * ROWS), :]


def stack(kva, kvb, kvb2, kvc):
    return pl.pallas_call(
        stack_kernel,
        in_specs=[WHOLE] * 4,
        out_specs=[WHOLE] * 2,
        out_shape=[
            jax.ShapeDtypeStruct((3 * ROWS, 2 * HD), BF),
            jax.ShapeDtypeStruct((2 * ROWS, 2 * HD), BF),
        ],
        compiler_params=params(8),
        name="stack",
    )(kva, kvb, kvb2, kvc)


def token_kernel(seg, e, docs, q_ref, kvs, far_kvs, o_ref, kcode):
    x, y, _, _ = place()
    lane = lax.broadcasted_iota(jnp.int32, (1, ROWS), 1).astype(F32)

    def codes_of(block):
        start = jnp.maximum(block, 0) * ROWS
        doc = docs[seg : seg + 1, pl.ds(pl.multiple_of(start, ROWS), ROWS)].astype(F32)
        return doc * 4096.0, doc * 4096.0 + lane + start.astype(F32)

    first_row = jnp.where(x >= 2, y - 1, y - 2)
    blocks = [(y - 2 + n) * SHAPE + x for n in range(3)]
    blocks += [(first_row + n) * SHAPE + (SHAPE - 1 - x) for n in range(2)]
    for n, block in enumerate(blocks):
        code = codes_of(block)[1]
        kcode[:, n * ROWS : (n + 1) * ROWS] = jnp.where(block >= 0, code, -1.0)
    near = lax.bitwise_xor(x, 1)
    low, high = codes_of(y * SHAPE + (x if e == 0 else near))
    low, high = column(low), column(high)
    if e == 0:
        span = slice(0, 3 * ROWS)
    else:
        span = pl.ds(pl.multiple_of(jnp.where(near < x, 0, ROWS), ROWS), 2 * ROWS)
    keys = [kvs[span, :], far_kvs[...]]
    codes = [kcode[:, span], kcode[:, 3 * ROWS :]]
    valid = [(k >= low) & (k <= high) for k in codes]
    for g in range(2):
        q = q_ref[:, g * HD : (g + 1) * HD]
        scores = [
            jnp.where(v, dot_t(q, k[:, :HD]) * LOG2E_SCALE, LOW) for v, k in zip(valid, keys)
        ]
        out, lse = attend(scores, [k[:, HD:] for k in keys])
        row = as_row(lse)
        hi = row.astype(BF).astype(F32)
        sub = lax.broadcasted_iota(jnp.int32, (16, ROWS), 0)
        stats = jnp.where(sub == 0, hi, jnp.where(sub == 1, row - hi, 0.0))
        o_ref[:ROWS, g * HD : (g + 1) * HD] = out.astype(BF)
        o_ref[ROWS:, g * HD : (g + 1) * HD] = stats.astype(BF)


def token_attention(docs, seg, e, q, kvs, far_kvs):
    return pl.pallas_call(
        functools.partial(token_kernel, seg, e),
        in_specs=[WHOLE] * 4,
        out_specs=WHOLE,
        out_shape=jax.ShapeDtypeStruct((ROWS + 16, 2 * HD), BF),
        scratch_shapes=[pltpu.VMEM((1, 5 * ROWS), F32)],
        compiler_params=params(16),
        cost_estimate=pl.CostEstimate(
            flops=3 * 10**9, bytes_accessed=4 * 10**6, transcendentals=10**6
        ),
        name="token_attention",
    )(docs, q, kvs, far_kvs)


def token_combine_kernel(q, qkvm, a, b, out_ref):
    refs = (a, b)
    for g in range(2):
        lanes = slice(g * HD, (g + 1) * HD)
        scores = dot_t(q[:, lanes], qkvm[:, 2 * HD : 3 * HD]) * LOG2E_SCALE
        out, lse = attend([scores], [qkvm[:, 3 * HD :]])
        outs, lses = [out], [lse]
        for r in refs:
            tail = r[ROWS:, lanes].astype(F32)
            lses.append(column(tail[0:1, :] + tail[1:2, :]))
            outs.append(r[:ROWS, lanes].astype(F32))
        peak = functools.reduce(jnp.maximum, lses)
        ws = [jnp.exp2(s - peak) for s in lses]
        mixed = sum(w * o for w, o in zip(ws, outs)) / sum(ws)
        out_ref[:, lanes] = mixed.astype(BF)


def token_combine(q, qkvm, parts):
    return pl.pallas_call(
        token_combine_kernel,
        in_specs=[WHOLE] * 4,
        out_specs=WHOLE,
        out_shape=jax.ShapeDtypeStruct((ROWS, 2 * HD), BF),
        compiler_params=params(12),
        cost_estimate=pl.CostEstimate(flops=5 * 10**8, bytes_accessed=10**6, transcendentals=4096),
        name="token_combine",
    )(q, qkvm, *parts)


def token_out_kernel(seg, *refs):
    blocks, cols, w_out, out_ref, flat = refs[:6], *refs[6:]
    acc = features(cols, seg, flat)
    for h, v in zip(gathered_heads(), block_values(blocks)):
        acc = acc + dot_t(w_out[:, pl.ds(pl.multiple_of(h * 2 * HD, 2 * HD), 2 * HD)], v)
    out_ref[0] = acc.astype(BF)


def features(cols, seg, flat):
    _, _, _, c = place()
    for at in range(0, 512, 128):
        flat[at : at + 128, :] = cols[seg, :, at : at + 128].astype(F32).T
    return flat[pl.ds(pl.multiple_of(c * 64, 64), COLS), :]


def token_out(blocks, cols, seg, w_out):
    return pl.pallas_call(
        functools.partial(token_out_kernel, seg),
        grid=(1,),
        in_specs=[WHOLE] * 8,
        out_specs=pl.BlockSpec((1, COLS, ROWS), lambda k: (seg, 0, 0)),
        out_shape=jax.ShapeDtypeStruct((2, COLS, ROWS), BF),
        scratch_shapes=[pltpu.VMEM((512, ROWS), F32)],
        compiler_params=params(12),
        cost_estimate=pl.CostEstimate(
            flops=2 * ROWS * 4096 * COLS, bytes_accessed=6 * 10**6, transcendentals=0
        ),
        name="token_out",
    )(*blocks, cols, w_out)


def early_kernel(seg, *refs):
    cols, w_out, out_ref, flat = refs[4:]
    own, swapped, near, near2 = refs[:4]
    values = [own[...], swapped[...], near[0], near[1], near2[0], near2[1]]
    acc = features(cols, seg, flat)
    for h, v in zip(gathered_heads(), values):
        acc = acc + dot_t(w_out[:, pl.ds(pl.multiple_of(h * 2 * HD, 2 * HD), 2 * HD)], v)
    out_ref[...] = acc


def token_out_early(blocks, cols, seg, w_out):
    return pl.pallas_call(
        functools.partial(early_kernel, seg),
        in_specs=[WHOLE] * 6,
        out_specs=WHOLE,
        out_shape=jax.ShapeDtypeStruct((COLS, ROWS), F32),
        scratch_shapes=[pltpu.VMEM((512, ROWS), F32)],
        compiler_params=params(12),
        cost_estimate=pl.CostEstimate(
            flops=2 * ROWS * 3072 * COLS, bytes_accessed=5 * 10**6, transcendentals=0
        ),
        name="token_out_early",
    )(*blocks, cols, w_out)


def late_kernel(far, far2, early, w_out, before, out_ref):
    acc = early[...]
    for h, v in zip(gathered_heads()[6:], (far[...], far2[...])):
        acc = acc + dot_t(w_out[:, pl.ds(pl.multiple_of(h * 2 * HD, 2 * HD), 2 * HD)], v)
    out_ref[0] = acc.astype(BF)


def token_out_late(far, far2, early, seg, w_out, before):
    return pl.pallas_call(
        late_kernel,
        grid=(1,),
        in_specs=[WHOLE] * 4 + [pl.BlockSpec(memory_space=pl.ANY)],
        out_specs=pl.BlockSpec((1, COLS, ROWS), lambda k: (seg, 0, 0)),
        out_shape=jax.ShapeDtypeStruct((2, COLS, ROWS), BF),
        input_output_aliases={4: 0},
        compiler_params=params(12),
        cost_estimate=pl.CostEstimate(
            flops=2 * ROWS * 1024 * COLS, bytes_accessed=3 * 10**6, transcendentals=0
        ),
        name="token_out_late",
    )(far, far2, early, w_out, before)


N_SEQ, N_HEAD = SHAPE * SHAPE, 8


def x_xor(v, d):
    return lax.ppermute(v, "seq", [(i, i ^ d) for i in range(N_SEQ)])


def y_xor(v, d):
    return x_xor(v, 4 * d)


def y_later(v):
    return lax.ppermute(v, "seq", [(i, i + SHAPE) for i in range(N_SEQ - SHAPE)])


def all_four(send, v):
    near = send(v, 1)
    return [v, near, send(near, 3), send(v, 3)]


def x_near(v):
    return lax.ppermute(v, "seq", [(i, i ^ 1) for i in range(N_SEQ)])


def x_far(v):
    return lax.ppermute(v, "seq", [(i, i ^ 3) for i in range(N_SEQ)])


def y_near(v):
    return lax.ppermute(v, "seq", [(i, i ^ 4) for i in range(N_SEQ)])


def y_far(v):
    return lax.ppermute(v, "seq", [(i, i ^ 12) for i in range(N_SEQ)])


def z_xor(v, d):
    return lax.ppermute(v, "head", [(i, i ^ (2 * d)) for i in range(N_HEAD)])


def z_turn(v):
    return lax.ppermute(v, "head", [(i, (i + 2 - 4 * (i % 2)) % N_HEAD) for i in range(N_HEAD)])


def other_core(v):
    return lax.ppermute(v, "head", [(i, i ^ 1) for i in range(N_HEAD)])


def add(a, b):
    return (a.astype(F32) + b.astype(F32)).astype(BF)


def gather_heads_direct(v):
    far = z_xor(v, 2)
    swapped = other_core(v)
    near = z_turn(pair_up(v, swapped))
    near2 = other_core(near)
    return v, swapped, near, near2, far, other_core(far)


def gather_heads(v):
    swapped = other_core(v)
    near = z_turn(pair_up(v, swapped))
    far = z_turn(first_of(near))
    near2 = other_core(near)
    return v, swapped, near, near2, far, other_core(far)


def memory_tail(attn, mem, w_out, proj):
    blocks = gather_heads_direct(attn)
    keep, send = memory_write(blocks, mem, w_out, proj)
    half = add(keep, other_core(send))
    near, far, two = [z_xor(half, d) for d in (1, 3, 2)]
    half = ((half.astype(F32) + near.astype(F32)) + (far.astype(F32) + two.astype(F32))).astype(BF)
    return half, other_core(half)


def per_device(segment_input, doc_ids, memory, gain, w_query, w_key, w_value, w_out, mem_proj):
    in_hbm = lambda v: pltpu.with_memory_space_constraint(v, pltpu.HBM)
    x = in_hbm(segment_input)

    q0, kv0, qkvm0, part, *weights = first_project(
        x, in_hbm(memory), gain, *[in_hbm(w) for w in (w_query, w_key, w_value)]
    )
    weights = (gain, *weights)
    q1, kv1, w_out, mem_proj, cols = second_project(x, *weights, in_hbm(w_out.T), in_hbm(mem_proj))

    part = memory_combine(part, x_near(part))
    part = memory_combine(part, x_far(part))
    part = memory_combine(part, y_near(part))
    attn = memory_combine(part, y_far(part), True)
    own, other = memory_tail(attn, memory, w_out, mem_proj)

    next_row = y_later(kv0)
    kvs0 = [kv0, next_row, y_later(next_row), next_row]
    kvs1 = all_four(y_xor, kv1)
    qkvm1, part, mem1 = memory_project(own, other, *weights, kvs1)
    part = memory_combine(part, x_near(part))
    attn = memory_combine(part, x_far(part), True)
    own, other = memory_tail(attn, mem1, w_out, mem_proj)

    for s, (kvs, qkvm) in enumerate(((kvs0, qkvm0), (kvs1, qkvm1))):
        own_q = (q0, q1)[s]
        near_q = x_xor(own_q, 1)
        stacked, send = stack(kvs[2], kvs[1], kvs[-1], kvs[0])
        far_kvs = x_xor(send, 3)
        keys = (stacked, far_kvs)
        send = token_attention(doc_ids, s, 1, near_q, *keys)
        mine = token_attention(doc_ids, s, 0, own_q, *keys)
        parts = [mine, x_xor(send, 1)]
        attn = token_combine(own_q, qkvm, parts)
        blocks = gather_heads(attn)
        if s == 0:
            hidden = token_out(blocks, cols, s, w_out)
        else:
            early = token_out_early(blocks[:4], cols, s, w_out)
            hidden = token_out_late(*blocks[4:], early, s, w_out, hidden)
    return hidden.transpose(0, 2, 1), finish(own, other)


def solution(mesh):
    return jax.shard_map(
        per_device,
        mesh=mesh,
        in_specs=(
            P(None, "seq", None),
            P(),
            P(),
            P(),
            P(None, "head"),
            P(None, "head"),
            P(None, "head"),
            P(None, "head"),
            P("head", None),
        ),
        out_specs=(P(None, "seq", "head"), P()),
        check_vma=False,
    )
```
